128 devices in a mesh: gx: 4 (over y), gy: 8 (over z, x_lo), gz: 4 (over x_hi, core).
Axes of the slice: x: 4 (x_hi: 2, x_lo: 2; x = x_hi * 2 + x_lo), y: 4, z: 4, core: 2. Of those that a mesh axis runs over, the one named last changes fastest.
Arguments:
- node_latent: bfloat16 [64, 256, 16, 128], P('gx', 'gy', 'gz'), may hold values from -6 to 6
- edge_latent: bfloat16 [4, 8, 4, 12288, 128], P('gx', 'gy', 'gz'), may hold values from -6 to 6
- senders: int32 [4, 8, 4, 12288], P('gx', 'gy', 'gz'), may hold values from 7 to 3664, as said below
- receivers: int32 [4, 8, 4, 12288], P('gx', 'gy', 'gz'), may hold values from 0 to 2047, as said below
- w1_edge: bfloat16 [384, 128], replicated, may hold values from -0.3125 to 0.3125
- b1_edge: float32 [128], replicated, may hold values from -3 to 3
- w2_edge: bfloat16 [128, 128], replicated, may hold values from -0.5 to 0.5
- b2_edge: float32 [128], replicated, may hold values from -3 to 3
- w1_node: bfloat16 [256, 128], replicated, may hold values from -0.375 to 0.375
- b1_node: float32 [128], replicated, may hold values from -3 to 3
- w2_node: bfloat16 [128, 128], replicated, may hold values from -0.5 to 0.5
- cot_node: bfloat16 [64, 256, 16, 128], P('gx', 'gy', 'gz'), may hold values from -6 to 6
- cot_edge: bfloat16 [4, 8, 4, 12288, 128], P('gx', 'gy', 'gz'), may hold values from -8 to 8
Outputs:
- grad_node: bfloat16 [64, 256, 16, 128], P('gx', 'gy', 'gz')
- grad_edge: bfloat16 [4, 8, 4, 12288, 128], P('gx', 'gy', 'gz')
- grad_w1_edge: float32 [384, 128], replicated
- grad_w2_edge: float32 [128, 128], replicated
- grad_w1_node: float32 [256, 128], replicated
- grad_w2_node: float32 [128, 128], replicated
- grad_biases: float32 [4, 128], replicated
The draws below stay inside these ranges and needn't reach their ends.
Inputs may be any that keep to these rules, and one draw needn't show every extreme that they name: `receivers`: in every block the list is nondecreasing; entry (i * 32 + j) * 4 + l names the block's cell at local coordinates (i, j, l). `senders`: entry (p * 34 + q) * 6 + r names the cell at local coordinates (p - 1, q - 1, r - 1) of the block extended by one cell on every side, the extension being cells of the adjacent blocks around the periodic box; it is always one of the six face neighbours of the same slot's receiver.
All inputs are finite; a program needn't handle non-finite values.
Results may differ from the reference program's by a relative error of at most 0.01.
Values may be sent and summed in bfloat16 or wider, within the bound.
No kernel may reach another device: no remote copies, remote signals or barrier semaphores. Data moves between devices by JAX's collectives and lax.ppermute only.
A program may use at most 128 MiB of HBM per device.

```python
import jax
import jax.numpy as jnp
from jax import lax

H = 128
BX = 16
BY = 32
BZ = 4
CELLS = 2048
EDGES_DEV = 12288
NX = 64
NY = 256
NZ = 16
PARAMS = 115200
N_GX = 4
N_GY = 8
N_GZ = 4


def edge_lists(key):
    base_key = jax.random.fold_in(key, 7)
    receiver_key, direction_key = jax.random.split(base_key)
    grid_shape = (N_GX, N_GY, N_GZ, EDGES_DEV)
    receiver_ids = jnp.sort(jax.random.randint(receiver_key, grid_shape, 0, BX * BY * BZ), axis=-1)
    direction = jax.random.randint(direction_key, grid_shape, 0, 6)
    along_x = receiver_ids // (BY * BZ)
    along_y = receiver_ids // BZ % BY
    along_z = receiver_ids % BZ
    step_x = (direction == 0).astype(jnp.int32) - (direction == 1).astype(jnp.int32)
    step_y = (direction == 2).astype(jnp.int32) - (direction == 3).astype(jnp.int32)
    step_z = (direction == 4).astype(jnp.int32) - (direction == 5).astype(jnp.int32)
    sender_ids = ((along_x + 1 + step_x) * (BY + 2) + along_y + 1 + step_y) * (BZ + 2) + along_z + 1 + step_z
    return (sender_ids.astype(jnp.int32), receiver_ids.astype(jnp.int32))


def draw_senders(key, part):
    return edge_lists(key)[0]


def draw_receivers(key, part):
    return edge_lists(key)[1]


def draw_cot_edge(key, part):
    base_key = jax.random.fold_in(key, 23)
    noise_key, common_key, scale_key = jax.random.split(base_key, 3)
    grid_shape = (N_GX, N_GY, N_GZ, EDGES_DEV, H)
    noise_part = jax.random.normal(noise_key, grid_shape, jnp.float32)
    values = noise_part
    return jnp.clip(values, -8.0, 8.0).astype(jnp.bfloat16)


def steps_of(rng, dims, pieces, smallest, top_value):
    def one(dim, parts):
        heights = jax.random.uniform(jax.random.fold_in(jax.random.fold_in(rng, 6), dim), (parts,), jnp.float32, smallest / len(pieces), top_value / len(pieces))
        return jnp.repeat(jnp.exp(heights), dims[dim] // parts).reshape((-1,) + (1,) * (len(dims) - dim - 1))

    loudness = one(*pieces[0])
    for cut in pieces[1:]:
        loudness = loudness * one(*cut)
    return loudness


def bell_draw(stream_key, dims, spread, reach, cuts=(), kind=jnp.bfloat16):
    array = spread * jax.random.normal(stream_key, dims, jnp.float32)
    if cuts:
        array = array * steps_of(stream_key, dims, cuts, -0.22, 0.18)
    return jnp.clip(array, -reach, reach).astype(kind)


def setup_inputs(seed: int = 0) -> dict:
    seeds = jax.random.split(jax.random.key(seed), 14)
    node_latent = bell_draw(seeds[0], (NX, NY, NZ, H), 1.0, 6.0, ((0, 4), (1, 8), (2, 4)))
    edge_latent = bell_draw(seeds[1], (N_GX, N_GY, N_GZ, EDGES_DEV, H), 1.0, 6.0, ((0, 4), (1, 8), (2, 4)))
    senders = draw_senders(jax.random.fold_in(seeds[13], 71), 0)
    receivers = draw_receivers(jax.random.fold_in(seeds[13], 71), 0)
    w1_edge = bell_draw(seeds[4], (3 * H, H), (3 * H) ** -0.5, 0.3125)
    b1_edge = bell_draw(seeds[5], (H,), 0.5, 3.0, (), jnp.float32)
    w2_edge = bell_draw(seeds[6], (H, H), H ** -0.5, 0.5)
    b2_edge = bell_draw(seeds[7], (H,), 0.5, 3.0, (), jnp.float32)
    w1_node = bell_draw(seeds[8], (2 * H, H), (2 * H) ** -0.5, 0.375)
    b1_node = bell_draw(seeds[9], (H,), 0.5, 3.0, (), jnp.float32)
    w2_node = bell_draw(seeds[10], (H, H), H ** -0.5, 0.5)
    cot_node = bell_draw(seeds[11], (NX, NY, NZ, H), 1.0, 6.0, ((0, 4), (1, 8), (2, 4)))
    cot_edge = draw_cot_edge(jax.random.fold_in(seeds[13], 71), 0)
    return dict(node_latent=node_latent, edge_latent=edge_latent, senders=senders, receivers=receivers, w1_edge=w1_edge, b1_edge=b1_edge, w2_edge=w2_edge, b2_edge=b2_edge, w1_node=w1_node, b1_node=b1_node, w2_node=w2_node, cot_node=cot_node, cot_edge=cot_edge)


def column_sums(values):
    return lax.optimization_barrier(jnp.sum(values.astype(jnp.float32), axis=0))

def silu_slope(values):
    sigma = jax.nn.sigmoid(values)
    return sigma * (1.0 + values * (1.0 - sigma))

def block_terms(padded, edge_rows, cot_rows, cot_cells, sender_ids, receiver_ids, w1_edge, b1_edge, w2_edge, b2_edge, w1_node, b1_node, w2_node):
    latent = edge_rows.shape[1]
    cell_count = cot_cells.shape[0]
    flat_pad = padded.reshape(-1, latent)
    own_rows = padded[1:-1, 1:-1, 1:-1].reshape(cell_count, latent)
    sender_rows = jnp.take(flat_pad, sender_ids, axis=0)
    receiver_rows = jnp.take(own_rows, receiver_ids, axis=0)
    x_edge = jnp.concatenate([edge_rows, sender_rows, receiver_rows], axis=1)
    z_edge = jnp.dot(x_edge, w1_edge, preferred_element_type=jnp.float32) + b1_edge
    u_edge = jax.nn.silu(z_edge).astype(jnp.bfloat16)
    edge_new = (edge_rows.astype(jnp.float32) + jnp.dot(u_edge, w2_edge, preferred_element_type=jnp.float32) + b2_edge).astype(jnp.bfloat16)
    aggregate = jax.ops.segment_sum(edge_new.astype(jnp.float32), receiver_ids, cell_count, indices_are_sorted=True).astype(jnp.bfloat16)
    x_node = jnp.concatenate([own_rows, aggregate], axis=1)
    z_node = jnp.dot(x_node, w1_node, preferred_element_type=jnp.float32) + b1_node
    u_node = jax.nn.silu(z_node).astype(jnp.bfloat16)
    dz_node = (jnp.dot(cot_cells, w2_node.T, preferred_element_type=jnp.float32) * silu_slope(z_node)).astype(jnp.bfloat16)
    dx_node = jnp.dot(dz_node, w1_node.T, preferred_element_type=jnp.float32)
    d_edge = (cot_rows.astype(jnp.float32) + jnp.take(dx_node[:, latent:], receiver_ids, axis=0)).astype(jnp.bfloat16)
    dz_edge = (jnp.dot(d_edge, w2_edge.T, preferred_element_type=jnp.float32) * silu_slope(z_edge)).astype(jnp.bfloat16)
    dx_edge = jnp.dot(dz_edge, w1_edge.T, preferred_element_type=jnp.float32)
    grad_edge = (d_edge.astype(jnp.float32) + dx_edge[:, :latent]).astype(jnp.bfloat16)
    receiver_sum = jax.ops.segment_sum(dx_edge[:, 2 * latent:], receiver_ids, cell_count, indices_are_sorted=True)
    sender_sum = jax.ops.segment_sum(dx_edge[:, latent:2 * latent], sender_ids, flat_pad.shape[0])
    local_rows = dx_node[:, :latent] + receiver_sum
    raws = (jnp.dot(x_edge.T, dz_edge, preferred_element_type=jnp.float32), column_sums(dz_edge), jnp.dot(u_edge.T, d_edge, preferred_element_type=jnp.float32), column_sums(d_edge), jnp.dot(x_node.T, dz_node, preferred_element_type=jnp.float32), column_sums(dz_node), jnp.dot(u_node.T, cot_cells, preferred_element_type=jnp.float32), column_sums(cot_cells))
    return (grad_edge, local_rows, sender_sum, raws)

def reference(node_latent, edge_latent, senders, receivers, w1_edge, b1_edge, w2_edge, b2_edge, w1_node, b1_node, w2_node, cot_node, cot_edge):
    block_total = N_GX * N_GY * N_GZ
    halo_grid = jnp.pad(node_latent, ((1, 1), (1, 1), (1, 1), (0, 0)), mode='wrap')
    edge_blocks = edge_latent.reshape(block_total, EDGES_DEV, H)
    cot_blocks = cot_edge.reshape(block_total, EDGES_DEV, H)
    sender_blocks = senders.reshape(block_total, EDGES_DEV)
    receiver_blocks = receivers.reshape(block_total, EDGES_DEV)
    zero_index = jnp.zeros((), jnp.int32)
    shapes = ((3 * H, H), (H,), (H, H), (H,), (2 * H, H), (H,), (H, H), (H,))
    totals = tuple((jnp.zeros(shape_item, jnp.float32) for shape_item in shapes))
    grad_grid = jnp.zeros((NX + 2, NY + 2, NZ + 2, H), jnp.float32)

    def block_step(running, inputs):
        grid_now, totals_now = running
        block_index, edge_rows, cot_rows, sender_ids, receiver_ids = inputs
        corner_x = (block_index // (N_GY * N_GZ) * BX).astype(jnp.int32)
        corner_y = (block_index // N_GZ % N_GY * BY).astype(jnp.int32)
        corner_z = (block_index % N_GZ * BZ).astype(jnp.int32)
        anchor = (corner_x, corner_y, corner_z, zero_index)
        padded = lax.dynamic_slice(halo_grid, anchor, (BX + 2, BY + 2, BZ + 2, H))
        cot_cells = lax.dynamic_slice(cot_node, anchor, (BX, BY, BZ, H)).reshape(CELLS, H)
        grad_edge, local_rows, sender_sum, raws = block_terms(padded, edge_rows, cot_rows, cot_cells, sender_ids, receiver_ids, w1_edge, b1_edge, w2_edge, b2_edge, w1_node, b1_node, w2_node)
        block_grad = sender_sum.reshape(BX + 2, BY + 2, BZ + 2, H)
        block_grad = block_grad.at[1:-1, 1:-1, 1:-1].add(local_rows.reshape(BX, BY, BZ, H))
        current = lax.dynamic_slice(grid_now, anchor, (BX + 2, BY + 2, BZ + 2, H))
        grid_now = lax.dynamic_update_slice(grid_now, current + block_grad, anchor)
        totals_now = tuple((older + fresh for older, fresh in zip(totals_now, raws)))
        return ((grid_now, totals_now), grad_edge)
    block_ids = jnp.arange(block_total, dtype=jnp.int32)
    (grad_grid, totals), edge_grads = lax.scan(block_step, (grad_grid, totals), (block_ids, edge_blocks, cot_blocks, sender_blocks, receiver_blocks))
    folded = grad_grid.at[1].add(grad_grid[-1]).at[-2].add(grad_grid[0])
    folded = folded.at[:, 1].add(folded[:, -1]).at[:, -2].add(folded[:, 0])
    folded = folded.at[:, :, 1].add(folded[:, :, -1]).at[:, :, -2].add(folded[:, :, 0])
    grad_node = (cot_node.astype(jnp.float32) + folded[1:-1, 1:-1, 1:-1]).astype(jnp.bfloat16)
    grad_edge = edge_grads.reshape(N_GX, N_GY, N_GZ, EDGES_DEV, H)
    squares = sum((jnp.sum(entry * entry) for entry in totals))
    factor = 1.0 / jnp.maximum(1.0, jnp.sqrt(squares / PARAMS))
    grad_w1_edge = totals[0] * factor
    grad_w2_edge = totals[2] * factor
    grad_w1_node = totals[4] * factor
    grad_w2_node = totals[6] * factor
    grad_biases = jnp.stack([totals[1], totals[3], totals[5], totals[7]]) * factor
    return (grad_node, grad_edge, grad_w1_edge, grad_w2_edge, grad_w1_node, grad_w2_node, grad_biases)
```

```python
import jax
import jax.numpy as jnp
from jax import lax
from jax.experimental import pallas as pl
from jax.experimental.pallas import tpu as pltpu
from jax.sharding import PartitionSpec as P

H = 128
PLANE = 128
N_PLANE = 16
CELLS = N_PLANE * PLANE
EDGES = 12288
TILE = 256
TILES = EDGES // TILE
WIN = 64
GROUP = 2
ROWS = CELLS + 128
PAD_ROWS = CELLS + 3 * PLANE
PARAM_ROWS = 1024
AXES = ("gx", "gy", "gz")
F32 = jnp.float32
BF16 = jnp.bfloat16


def dot(a, b):
    return lax.dot_general(a, b, (((1,), (0,)), ((), ())), preferred_element_type=F32)


def dot_first(a, b):
    return lax.dot_general(a, b, (((0,), (0,)), ((), ())), preferred_element_type=F32)


def flip(w):
    return w.astype(F32).T.astype(BF16)


def hot(mask):
    return jnp.where(mask, 1.0, 0.0).astype(BF16)


def iota(shape, dim):
    return lax.broadcasted_iota(jnp.int32, shape, dim)


def sigmoid(v):
    return 0.5 * jnp.tanh(0.5 * v) + 0.5


def layer_kernel(
    first_ref,
    last_ref,
    code_ref,
    node_ref,
    cotn_ref,
    xlo_ref,
    xhi_ref,
    ylo_ref,
    yhi_ref,
    zlo_ref,
    zhi_ref,
    e_ref,
    cot_ref,
    w1e_ref,
    b1e_ref,
    w2e_ref,
    b2e_ref,
    w1n_ref,
    b1n_ref,
    w2n_ref,
    gedge_ref,
    gown_ref,
    fx_ref,
    fy_ref,
    fz_ref,
    par_ref,
    own_ref,
    zx_ref,
    yx_ref,
    ppad_ref,
    tab_ref,
    col_ref,
    u_ref,
    slope_ref,
    eu_ref,
    deg_ref,
    dd_ref,
    spad_ref,
    acc_ref,
    wide_ref,
    zacc_ref,
    const_ref,
    flip_ref,
    sr_ref,
):
    w1a = w1e_ref[0:H]
    w1b = w1e_ref[H : 2 * H]
    w1c = w1e_ref[2 * H : 3 * H]
    par_ref[...] = jnp.zeros(par_ref.shape, F32)
    eu_ref[...] = jnp.zeros(eu_ref.shape, F32)
    deg_ref[...] = jnp.zeros(deg_ref.shape, F32)
    spad_ref[...] = jnp.zeros(spad_ref.shape, F32)
    acc_ref[...] = jnp.zeros(acc_ref.shape, F32)
    dd_ref[CELLS:ROWS] = jnp.zeros((ROWS - CELLS, 2 * H), BF16)
    tab_ref[:, CELLS:ROWS] = jnp.zeros((5, ROWS - CELLS, H), BF16)
    ppad_ref[CELLS + 2 * PLANE :] = jnp.zeros((PAD_ROWS - CELLS - 2 * PLANE, H), BF16)
    const_ref[:, 0:H] = flip(w2e_ref[...])
    const_ref[:, H:] = hot(iota((H, H), 0) == iota((H, H), 1))
    flip_ref[0:H] = flip(w1b)
    flip_ref[H : 2 * H] = flip(w1c)
    flip_ref[2 * H : 3 * H] = flip(w1a)

    ppad_ref[0:PLANE] = dot(xlo_ref[...], w1b).astype(BF16)
    ppad_ref[CELLS + PLANE : CELLS + 2 * PLANE] = dot(xhi_ref[...], w1b).astype(BF16)
    yx_ref[0:PLANE] = dot(ylo_ref[...], w1b)
    yx_ref[PLANE : 2 * PLANE] = dot(yhi_ref[...], w1b)
    zx_ref[pl.ds(0, CELLS // 4, 4), :] = dot(zlo_ref[...], w1b)
    zx_ref[pl.ds(3, CELLS // 4, 4), :] = dot(zhi_ref[...], w1b)
    w1bc = jnp.concatenate([w1b, w1c], axis=1)
    row = iota((PLANE, H), 0)
    at_low = (row & 3) == 0
    at_high = (row & 3) == 3

    def prepare(i, carry):
        base = pl.multiple_of(i * PLANE, PLANE)
        both = dot(node_ref[pl.ds(base, PLANE), :], w1bc)
        p = both[:, 0:H]
        tab_ref[4, pl.ds(base, PLANE), :] = (both[:, H:] + b1e_ref[...]).astype(BF16)
        ppad_ref[pl.ds(base + PLANE, PLANE), :] = p.astype(BF16)
        ylow = yx_ref[pl.ds(pl.multiple_of(i * 8, 8), 8), :]
        yhigh = yx_ref[pl.ds(pl.multiple_of(PLANE + i * 8, 8), 8), :]
        pad = jnp.zeros((PLANE - 8, H), F32)
        low_full = jnp.concatenate([ylow, pad], axis=0)
        high_full = jnp.concatenate([pad, yhigh], axis=0)
        up = jnp.where(row < PLANE - 4, pltpu.roll(p, PLANE - 4, 0), pltpu.roll(high_full, 4, 0))
        down = jnp.where(row >= 4, pltpu.roll(p, 4, 0), pltpu.roll(low_full, PLANE - 4, 0))
        tab_ref[0, pl.ds(base, PLANE), :] = up.astype(BF16)
        tab_ref[1, pl.ds(base, PLANE), :] = down.astype(BF16)
        zx = zx_ref[pl.ds(base, PLANE), :]
        tab_ref[2, pl.ds(base, PLANE), :] = jnp.where(
            at_high, zx, pltpu.roll(p, PLANE - 1, 0)
        ).astype(BF16)
        tab_ref[3, pl.ds(base, PLANE), :] = jnp.where(at_low, zx, pltpu.roll(p, 1, 0)).astype(BF16)
        return carry

    lax.fori_loop(0, N_PLANE, prepare, 0)

    lane = iota((TILE, H), 1)
    lane_code = (lane >> 6) * 4096 + (lane & 63)
    lane_self = jnp.where(lane < WIN, lane, -(1 << 20))
    srow = iota((H, TILE), 0)
    srow_code = (srow >> 6) * 4096 + (srow & 63)
    wrow = iota((WIN, TILE), 0)

    def start_of(t):
        return pl.multiple_of((first_ref[t] >> 4) << 4, 16)

    def windows_of(t):
        return ((last_ref[t] - start_of(t)) >> 6) + 1

    def rows_of(t):
        return pl.ds(pl.multiple_of(t * TILE, TILE), TILE)

    def columns(t):
        line = code_ref[pl.ds(t, 1), :].astype(F32)
        parts = [
            jnp.broadcast_to(line[:, k * H : (k + 1) * H], (H, H)).T for k in range(TILE // H)
        ]
        return jnp.concatenate(parts, axis=0).astype(jnp.int32)

    def gather_pre(col, w):
        shifted = col - w
        inner = (col & 4095) - w
        parts = [hot(shifted == lane_code + k * 8192) for k in range(3)]
        left = jnp.concatenate(parts + [hot(inner == lane_self)], axis=1)
        right = jnp.concatenate(
            [
                ppad_ref[pl.ds(w + 2 * PLANE, WIN), :],
                ppad_ref[pl.ds(w, WIN), :],
            ]
            + [tab_ref[k, pl.ds(w, WIN), :] for k in range(5)]
            + [jnp.zeros((WIN, H), BF16)],
            axis=0,
        )
        return dot(left, right)

    def activate(t, z):
        s = sigmoid(z)
        u = z * s
        ub = u.astype(BF16)
        u_ref[rows_of(t), :] = ub
        slope_ref[rows_of(t), :] = (s + u * (1.0 - s)).astype(BF16)
        return ub

    def collect(t, w, eu):
        picked = ((code_ref[pl.ds(t, 1), :] & 4095) - w) == wrow
        ones = jnp.where(picked, 1.0, 0.0)
        eu_ref[pl.ds(w, WIN), :] += dot(ones.astype(BF16), eu)
        deg_ref[pl.ds(w, WIN), :] += jnp.broadcast_to(
            jnp.sum(ones, axis=1, keepdims=True), (WIN, H)
        )

    def forward_fast(t):
        col = columns(t)
        col_ref[rows_of(t), :] = col
        e = e_ref[rows_of(t), :]
        w = start_of(t)
        ub = activate(t, gather_pre(col, w) + dot(e, w1a))
        collect(t, w, jnp.concatenate([e, ub], axis=1))

    def forward_slow(t):
        col_ref[rows_of(t), :] = columns(t)
        zacc_ref[:, 0:H] = dot(e_ref[rows_of(t), :], w1a)

        def more(k, carry):
            w = pl.multiple_of(start_of(t) + k * WIN, 16)
            zacc_ref[:, 0:H] += gather_pre(col_ref[rows_of(t), :], w)
            return carry

        lax.fori_loop(0, windows_of(t), more, 0)
        activate(t, zacc_ref[:, 0:H])

        def put(k, carry):
            w = pl.multiple_of(start_of(t) + k * WIN, 16)
            collect(t, w, jnp.concatenate([e_ref[rows_of(t), :], u_ref[rows_of(t), :]], axis=1))
            return carry

        lax.fori_loop(0, windows_of(t), put, 0)

    def each_group(fast, slow):
        def body(g, carry):
            tiles = [g * GROUP + k for k in range(GROUP)]
            fits = windows_of(tiles[0]) <= 1
            for t in tiles[1:]:
                fits = jnp.logical_and(fits, windows_of(t) <= 1)

            @pl.when(fits)
            def _():
                for t in tiles:
                    fast(t)

            @pl.when(jnp.logical_not(fits))
            def _():
                for t in tiles:
                    slow(t)

            return carry

        lax.fori_loop(0, TILES // GROUP, body, 0)

    each_group(forward_fast, forward_slow)

    w2n_flip = flip(w2n_ref[...])
    w1n_flip = jnp.concatenate([flip(w1n_ref[0:H]), flip(w1n_ref[H : 2 * H])], axis=1)

    def cells(k, carry):
        at = pl.ds(pl.multiple_of(k * TILE, TILE), TILE)
        eu = eu_ref[at, :]
        usum = eu[:, H:]
        uh = usum.astype(BF16)
        ul = (usum - uh.astype(F32)).astype(BF16)
        w2 = w2e_ref[...]
        agg = (eu[:, 0:H] + deg_ref[at, :] * b2e_ref[...]) + dot(
            jnp.concatenate([uh, ul], axis=1), jnp.concatenate([w2, w2], axis=0)
        )
        x = jnp.concatenate([node_ref[at, :], agg.astype(BF16)], axis=1)
        z = dot(x, w1n_ref[...]) + b1n_ref[...]
        s = sigmoid(z)
        u = z * s
        cot = cotn_ref[at, :]
        dz = (dot(cot, w2n_flip) * (s + u * (1.0 - s))).astype(BF16)
        dx = dot(dz, w1n_flip)
        cot32 = cot.astype(F32)
        gown_ref[at, :] = cot32 + dx[:, 0:H]
        dagg = dx[:, H:].astype(BF16)
        dd_ref[at, 0:H] = dot(dagg, const_ref[:, 0:H]).astype(BF16)
        dd_ref[at, H:] = dagg
        par_ref[4 * H : 6 * H, :] += dot_first(x, dz)
        par_ref[6 * H : 7 * H, :] += dot_first(u.astype(BF16), cot)
        par_ref[7 * H + 2 : 7 * H + 3, :] += jnp.sum(dz.astype(F32), axis=0, keepdims=True)
        par_ref[7 * H + 3 : 7 * H + 4, :] += jnp.sum(cot32, axis=0, keepdims=True)
        return carry

    lax.fori_loop(0, CELLS // TILE, cells, 0)

    def spread(col, w, cot):
        left = jnp.concatenate([hot((col & 4095) - w == lane), cot], axis=1)
        right = jnp.concatenate([dd_ref[pl.ds(w, H), :], const_ref[...]], axis=0)
        return dot(left, right)

    def scatter(t, w, dz):
        shifted = code_ref[pl.ds(t, 1), :] - w
        inner = (code_ref[pl.ds(t, 1), :] & 4095) - w
        parts = [hot(shifted == srow_code + k * 8192) for k in range(3)]
        sums = dot(jnp.concatenate(parts + [hot(inner == wrow)], axis=0), dz)
        spad_ref[pl.ds(w + 2 * PLANE, WIN), :] += sums[0:WIN]
        spad_ref[pl.ds(w, WIN), :] += sums[WIN : 2 * WIN]
        for k in range(5):
            acc_ref[k, pl.ds(w, WIN), :] += sums[(k + 2) * WIN : (k + 3) * WIN]

    def finish_edges(t, dd):
        d32 = dd[:, H:]
        d = d32.astype(BF16)
        d32 = d.astype(F32)
        dz = (dd[:, 0:H] * slope_ref[rows_of(t), :].astype(F32)).astype(BF16)
        gedge_ref[rows_of(t), :] = (d32 + dot(dz, flip_ref[2 * H : 3 * H])).astype(BF16)
        wide_ref[0:H, :] += dot_first(e_ref[rows_of(t), :], dz)
        wide_ref[H : 2 * H, :] += dot_first(u_ref[rows_of(t), :], d)
        wide_ref[2 * H : 2 * H + 8, :] += jnp.sum(d32.reshape(TILE // 8, 8, H), axis=0)
        return dz

    def backward_fast(t):
        w = start_of(t)
        dz = finish_edges(t, spread(col_ref[rows_of(t), :], w, cot_ref[rows_of(t), :]))
        scatter(t, w, dz)

    def backward_slow(t):
        zacc_ref[...] = dot(cot_ref[rows_of(t), :], const_ref[...])

        def more(k, carry):
            w = pl.multiple_of(start_of(t) + k * H, 16)
            zacc_ref[...] += spread(
                col_ref[rows_of(t), :], w, jnp.zeros((TILE, H), BF16)
            )
            return carry

        lax.fori_loop(0, (windows_of(t) + 1) >> 1, more, 0)
        own_ref[...] = finish_edges(t, zacc_ref[...])

        def put(k, carry):
            scatter(t, pl.multiple_of(start_of(t) + k * WIN, 16), own_ref[...])
            return carry

        lax.fori_loop(0, windows_of(t), put, 0)

    wide_ref[...] = jnp.zeros(wide_ref.shape, F32)
    each_group(backward_fast, backward_slow)

    row8 = iota((8, H), 0)

    def gather_cells(i, carry):
        base = pl.multiple_of(i * PLANE, PLANE)
        at = pl.ds(base, PLANE)
        yp = acc_ref[0, at, :]
        ym = acc_ref[1, at, :]
        zp = acc_ref[2, at, :]
        zm = acc_ref[3, at, :]
        zero = jnp.zeros((PLANE, H), F32)
        total = spad_ref[pl.ds(base + PLANE, PLANE), :]
        total += jnp.where(row >= 4, pltpu.roll(yp, 4, 0), zero)
        total += jnp.where(row < PLANE - 4, pltpu.roll(ym, PLANE - 4, 0), zero)
        total += jnp.where(at_low, zero, pltpu.roll(zp, 1, 0))
        total += jnp.where(at_high, zero, pltpu.roll(zm, PLANE - 1, 0))
        sr = jnp.concatenate([total, acc_ref[4, at, :]], axis=1)
        par_ref[7 * H : 7 * H + 1, :] += jnp.sum(acc_ref[4, at, :], axis=0, keepdims=True)
        sr16 = sr.astype(BF16)
        sr_ref[at, :] = sr16
        gown_ref[at, :] += dot(sr16, flip_ref[0 : 2 * H])
        eight = pl.multiple_of(i * 8, 8)
        yx_ref[pl.ds(eight, 8), :] = jnp.where(row8 >= 4, pltpu.roll(ym[0:8], 4, 0), 0.0)
        yx_ref[pl.ds(PLANE + eight, 8), :] = jnp.where(
            row8 < 4, pltpu.roll(yp[PLANE - 8 :], 4, 0), 0.0
        )
        return carry

    lax.fori_loop(0, N_PLANE, gather_cells, 0)
    both = dot_first(node_ref[...], sr_ref[...])
    w1b_flip = flip_ref[0:H]
    sx_lo = spad_ref[0:PLANE].astype(BF16)
    sx_hi = spad_ref[CELLS + PLANE : CELLS + 2 * PLANE].astype(BF16)
    sy_lo = yx_ref[0:PLANE].astype(BF16)
    sy_hi = yx_ref[PLANE : 2 * PLANE].astype(BF16)
    zx_ref[...] = acc_ref[3, 0:CELLS, :]
    sz_lo = zx_ref[pl.ds(0, CELLS // 4, 4), :].astype(BF16)
    zx_ref[...] = acc_ref[2, 0:CELLS, :]
    sz_hi = zx_ref[pl.ds(3, CELLS // 4, 4), :].astype(BF16)
    fx_ref[0] = dot(sx_lo, w1b_flip).astype(BF16)
    fx_ref[1] = dot(sx_hi, w1b_flip).astype(BF16)
    fy_ref[0] = dot(sy_lo, w1b_flip).astype(BF16)
    fy_ref[1] = dot(sy_hi, w1b_flip).astype(BF16)
    fz_ref[0] = dot(sz_lo, w1b_flip).astype(BF16)
    fz_ref[1] = dot(sz_hi, w1b_flip).astype(BF16)
    halo_x = dot_first(xlo_ref[...], sx_lo) + dot_first(xhi_ref[...], sx_hi)
    halo_y = dot_first(ylo_ref[...], sy_lo) + dot_first(yhi_ref[...], sy_hi)
    halo_z = dot_first(zlo_ref[...], sz_lo) + dot_first(zhi_ref[...], sz_hi)
    par_ref[0:H, :] = wide_ref[0:H, :]
    par_ref[H : 2 * H, :] = both[:, 0:H] + halo_x + halo_y + halo_z
    par_ref[2 * H : 3 * H, :] = both[:, H:]
    par_ref[3 * H : 4 * H, :] = wide_ref[H : 2 * H, :]
    par_ref[7 * H + 1 : 7 * H + 2, :] = jnp.sum(
        wide_ref[2 * H : 2 * H + 8, :], axis=0, keepdims=True
    )


def layer_call(first, last, code, *arrays):
    smem = pl.BlockSpec(memory_space=pltpu.SMEM)
    vmem = pl.BlockSpec(memory_space=pltpu.VMEM)
    return pl.pallas_call(
        layer_kernel,
        in_specs=[smem, smem] + [vmem] * 18,
        out_specs=[vmem] * 6,
        out_shape=[
            jax.ShapeDtypeStruct((EDGES, H), BF16),
            jax.ShapeDtypeStruct((CELLS, H), F32),
            jax.ShapeDtypeStruct((2, PLANE, H), BF16),
            jax.ShapeDtypeStruct((2, PLANE, H), BF16),
            jax.ShapeDtypeStruct((2, CELLS // 4, H), BF16),
            jax.ShapeDtypeStruct((PARAM_ROWS, H), F32),
        ],
        scratch_shapes=[
            pltpu.VMEM((TILE, H), BF16),
            pltpu.VMEM((CELLS, H), F32),
            pltpu.VMEM((2 * PLANE, H), F32),
            pltpu.VMEM((PAD_ROWS, H), BF16),
            pltpu.VMEM((5, ROWS, H), BF16),
            pltpu.VMEM((EDGES, H), jnp.int32),
            pltpu.VMEM((EDGES, H), BF16),
            pltpu.VMEM((EDGES, H), BF16),
            pltpu.VMEM((ROWS, 2 * H), F32),
            pltpu.VMEM((ROWS, H), F32),
            pltpu.VMEM((ROWS, 2 * H), BF16),
            pltpu.VMEM((PAD_ROWS, H), F32),
            pltpu.VMEM((5, ROWS, H), F32),
            pltpu.VMEM((2 * H + 8, H), F32),
            pltpu.VMEM((TILE, 2 * H), F32),
            pltpu.VMEM((H, 2 * H), BF16),
            pltpu.VMEM((3 * H, H), BF16),
            pltpu.VMEM((CELLS, 2 * H), BF16),
        ],
        compiler_params=pltpu.CompilerParams(vmem_limit_bytes=60 * 1024 * 1024),
        name="layer",
    )(first, last, code, *arrays)


def finish_kernel(
    gown_ref,
    xlo_ref,
    xhi_ref,
    ylo_ref,
    yhi_ref,
    zlo_ref,
    zhi_ref,
    par_ref,
    gnode_ref,
    w1e_ref,
    w2e_ref,
    w1n_ref,
    w2n_ref,
    bias_ref,
    sum_ref,
):
    par = par_ref[0 : 7 * H + 8, :]
    square = jnp.sum(par * par)
    factor = 1.0 / jnp.maximum(1.0, jnp.sqrt(jnp.full((1, H), square / (7 * H * H + 4 * H), F32)))
    w1e_ref[...] = par_ref[0 : 3 * H, :] * factor
    w2e_ref[...] = par_ref[3 * H : 4 * H, :] * factor
    w1n_ref[...] = par_ref[4 * H : 6 * H, :] * factor
    w2n_ref[...] = par_ref[6 * H : 7 * H, :] * factor
    bias_ref[...] = par_ref[7 * H : 7 * H + 4, :] * factor
    sum_ref[...] = gown_ref[...]
    sum_ref[0:PLANE] += xlo_ref[...].astype(F32)
    sum_ref[CELLS - PLANE :] += xhi_ref[...].astype(F32)
    for i in range(N_PLANE):
        low = ylo_ref[i * 8 : i * 8 + 8, :].astype(F32)
        high = yhi_ref[i * 8 : i * 8 + 8, :].astype(F32)
        sum_ref[i * PLANE : i * PLANE + 8, :] += low
        sum_ref[(i + 1) * PLANE - 8 : (i + 1) * PLANE, :] += high
    sum_ref[pl.ds(0, CELLS // 4, 4), :] += zlo_ref[...].astype(F32)
    sum_ref[pl.ds(3, CELLS // 4, 4), :] += zhi_ref[...].astype(F32)
    gnode_ref[...] = sum_ref[...].astype(BF16)


def finish_call(*arrays):
    return pl.pallas_call(
        finish_kernel,
        in_specs=[pl.BlockSpec(memory_space=pltpu.VMEM)] * 8,
        out_specs=[pl.BlockSpec(memory_space=pltpu.VMEM)] * 6,
        out_shape=[
            jax.ShapeDtypeStruct((CELLS, H), BF16),
            jax.ShapeDtypeStruct((3 * H, H), F32),
            jax.ShapeDtypeStruct((H, H), F32),
            jax.ShapeDtypeStruct((2 * H, H), F32),
            jax.ShapeDtypeStruct((H, H), F32),
            jax.ShapeDtypeStruct((4, H), F32),
        ],
        scratch_shapes=[pltpu.VMEM((CELLS, H), F32)],
        name="finish",
    )(*arrays)


def from_previous(value, axis):
    n = lax.axis_size(axis)
    return lax.ppermute(value, axis, [(k, (k + 1) % n) for k in range(n)])


def from_next(value, axis):
    n = lax.axis_size(axis)
    return lax.ppermute(value, axis, [((k + 1) % n, k) for k in range(n)])


def edge_codes(senders, receivers):
    r = receivers.reshape(TILES, TILE)
    s = senders.reshape(TILES, TILE)
    home = ((r >> 7) + 1) * 204 + (((r >> 2) & 31) + 1) * 6 + (r & 3) + 1
    delta = s - home
    size = jnp.abs(delta)
    side = jnp.where(size == 204, 0, jnp.where(size == 6, 2, 4)) + (delta < 0).astype(jnp.int32)
    return r[:, 0], r[:, -1], side * 4096 + r


def sum_over_devices(rows):
    count = 1
    for axis in AXES:
        count *= lax.axis_size(axis)
    chunks = rows.reshape(count, -1, H)
    mine = jnp.sum(lax.all_to_all(chunks, AXES, 0, 0, tiled=True), axis=0)
    copies = jnp.broadcast_to(mine[None], (count,) + mine.shape)
    return lax.all_to_all(copies, AXES, 0, 0, tiled=True).reshape(-1, H)


def on_device(
    node_latent,
    edge_latent,
    senders,
    receivers,
    w1_edge,
    b1_edge,
    w2_edge,
    b2_edge,
    w1_node,
    b1_node,
    w2_node,
    cot_node,
    cot_edge,
):
    zlo = from_previous(node_latent[:, :, 3], "gz").reshape(-1, H)
    zhi = from_next(node_latent[:, :, 0], "gz").reshape(-1, H)
    ylo = from_previous(node_latent[:, 30:32], "gy").reshape(-1, H)
    yhi = from_next(node_latent[:, 0:2], "gy").reshape(-1, H)
    xlo = from_previous(node_latent[15], "gx").reshape(-1, H)
    xhi = from_next(node_latent[0], "gx").reshape(-1, H)
    first, last, code = edge_codes(senders, receivers)
    gedge, gown, fx, fy, fz, par = layer_call(
        first,
        last,
        code,
        node_latent.reshape(CELLS, H),
        cot_node.reshape(CELLS, H),
        xlo,
        xhi,
        ylo,
        yhi,
        zlo,
        zhi,
        edge_latent.reshape(EDGES, H),
        cot_edge.reshape(EDGES, H),
        w1_edge,
        b1_edge.reshape(1, H),
        w2_edge,
        b2_edge.reshape(1, H),
        w1_node,
        b1_node.reshape(1, H),
        w2_node,
    )
    full = sum_over_devices(par)
    gnode, gw1e, gw2e, gw1n, gw2n, gbias = finish_call(
        gown,
        from_previous(fx[1], "gx"),
        from_next(fx[0], "gx"),
        from_previous(fy[1], "gy"),
        from_next(fy[0], "gy"),
        from_previous(fz[1], "gz"),
        from_next(fz[0], "gz"),
        full,
    )
    return (
        gnode.reshape(node_latent.shape),
        gedge.reshape(edge_latent.shape),
        gw1e,
        gw2e,
        gw1n,
        gw2n,
        gbias,
    )


def solution(mesh):
    cells = P("gx", "gy", "gz", None)
    edges = P("gx", "gy", "gz", None, None)
    return jax.shard_map(
        on_device,
        mesh=mesh,
        in_specs=(cells, edges, cells, cells) + (P(),) * 7 + (cells, edges),
        out_specs=(cells, edges) + (P(),) * 5,
        check_vma=False,
    )
```

```python
import jax
import jax.numpy as jnp
from jax import lax
from jax.experimental import pallas as pl
from jax.experimental.pallas import tpu as pltpu
from jax.sharding import PartitionSpec as P

H = 128
PLANE = 128
N_PLANE = 16
CELLS = N_PLANE * PLANE
EDGES = 12288
TILE = 256
TILES = EDGES // TILE
WIN = 64
MID = 128
GROUP = 2
HALF = TILE // H
CHUNKS = 4
ROWS = CELLS + 128
STRIDE = 208
GRID = N_PLANE * STRIDE + 128
PAD_ROWS = CELLS + 3 * PLANE
PARAM_ROWS = 1024
AXES = ("gx", "gy", "gz")
F32 = jnp.float32
BF16 = jnp.bfloat16


def dot(a, b):
    return lax.dot_general(a, b, (((1,), (0,)), ((), ())), preferred_element_type=F32)


def dot_first(a, b):
    return lax.dot_general(a, b, (((0,), (0,)), ((), ())), preferred_element_type=F32)


def flip(w):
    return w.astype(F32).T.astype(BF16)


def hot(mask):
    return jnp.where(mask, 1.0, 0.0).astype(BF16)


def iota(shape, dim):
    return lax.broadcasted_iota(jnp.int32, shape, dim)


def sigmoid(v):
    return 0.5 * jnp.tanh(0.5 * v) + 0.5


def layer_kernel(
    near_ref,
    send_ref,
    recv_ref,
    node_ref,
    cotn_ref,
    xlo_ref,
    xhi_ref,
    ylo_ref,
    yhi_ref,
    zlo_ref,
    zhi_ref,
    e_hbm,
    cot_hbm,
    w1e_ref,
    b1e_ref,
    w2e_ref,
    b2e_ref,
    w1n_ref,
    b1n_ref,
    w2n_ref,
    gedge_hbm,
    gown_ref,
    fx_ref,
    fy_ref,
    fz_ref,
    par_ref,
    e_ref,
    cot_ref,
    gedge_ref,
    dz_ref,
    own_ref,
    zx_ref,
    yx_ref,
    ppad_ref,
    home_ref,
    mid_ref,
    code_ref,
    col_ref,
    u_ref,
    slope_ref,
    eu_ref,
    deg_ref,
    dd_ref,
    spad_ref,
    rsum_ref,
    smid_ref,
    wide_ref,
    zacc_ref,
    const_ref,
    flip_ref,
    sr_ref,
    in_sem,
    out_sem,
):
    copy_e = pltpu.make_async_copy(e_hbm, e_ref, in_sem.at[0])
    copy_cot = pltpu.make_async_copy(cot_hbm, cot_ref, in_sem.at[1])
    copy_e.start()
    copy_cot.start()

    def copy_out(c):
        size = EDGES // CHUNKS
        at = pl.ds(pl.multiple_of(c * size, size), size)
        return pltpu.make_async_copy(gedge_ref.at[at, :], gedge_hbm.at[at, :], out_sem.at[c])

    w1a = w1e_ref[0:H]
    w1b = w1e_ref[H : 2 * H]
    w1c = w1e_ref[2 * H : 3 * H]
    par_ref[...] = jnp.zeros(par_ref.shape, F32)
    eu_ref[...] = jnp.zeros(eu_ref.shape, F32)
    deg_ref[...] = jnp.zeros(deg_ref.shape, F32)
    spad_ref[...] = jnp.zeros(spad_ref.shape, F32)
    rsum_ref[...] = jnp.zeros(rsum_ref.shape, F32)
    smid_ref[...] = jnp.zeros(smid_ref.shape, F32)
    mid_ref[...] = jnp.zeros(mid_ref.shape, F32)
    wide_ref[...] = jnp.zeros(wide_ref.shape, F32)
    dd_ref[CELLS:ROWS] = jnp.zeros((ROWS - CELLS, 2 * H), BF16)
    home_ref[CELLS:ROWS] = jnp.zeros((ROWS - CELLS, H), BF16)
    ppad_ref[CELLS + 2 * PLANE :] = jnp.zeros((PAD_ROWS - CELLS - 2 * PLANE, H), BF16)
    const_ref[:, 0:H] = flip(w2e_ref[...])
    const_ref[:, H:] = hot(iota((H, H), 0) == iota((H, H), 1))
    flip_ref[0:H] = flip(w1b)
    flip_ref[H : 2 * H] = flip(w1c)
    flip_ref[2 * H : 3 * H] = flip(w1a)

    r = recv_ref[...]
    s = send_ref[...]
    delta = s - (((r >> 7) + 1) * 204 + (((r >> 2) & 31) + 1) * 6 + (r & 3) + 1)
    inside = s - 204 + 4 * (r >> 7)
    place = jnp.where(delta == 204, r + 4096, jnp.where(delta == -204, r + 8192, inside))
    code_ref[...] = place * 2048 + r

    ppad_ref[0:PLANE] = dot(xlo_ref[...], w1b).astype(BF16)
    ppad_ref[CELLS + PLANE : CELLS + 2 * PLANE] = dot(xhi_ref[...], w1b).astype(BF16)
    yx_ref[0:PLANE] = dot(ylo_ref[...], w1b)
    yx_ref[PLANE : 2 * PLANE] = dot(yhi_ref[...], w1b)
    zx_ref[0] = dot(zlo_ref[...], w1b)
    zx_ref[1] = dot(zhi_ref[...], w1b)
    own_ref[...] = dot(node_ref[...], w1b)
    for i in range(N_PLANE):
        at = slice(i * PLANE, (i + 1) * PLANE)
        base = i * STRIDE
        ppad_ref[(i + 1) * PLANE : (i + 2) * PLANE] = own_ref[at].astype(BF16)
        home_ref[at] = (dot(node_ref[at], w1c) + b1e_ref[...]).astype(BF16)
        for l in range(4):
            mid_ref[pl.ds(base + 7 + l, 32, 6), :] = own_ref[pl.ds(i * PLANE + l, 32, 4), :]
        mid_ref[pl.ds(base + 6, 32, 6), :] = zx_ref[0, i * 32 : (i + 1) * 32, :]
        mid_ref[pl.ds(base + 11, 32, 6), :] = zx_ref[1, i * 32 : (i + 1) * 32, :]
        mid_ref[base + 1 : base + 5, :] = yx_ref[i * 8 + 4 : i * 8 + 8, :]
        mid_ref[base + 199 : base + 203, :] = yx_ref[PLANE + i * 8 : PLANE + i * 8 + 4, :]
    copy_e.wait()

    lane = iota((TILE, H), 1)
    lane_x = jnp.where(lane < WIN, 4096 + lane, 8192 - WIN + lane)
    lane_self = jnp.where(lane < WIN, lane, -(1 << 20))
    mrow = iota((MID, H), 0)
    wrow = iota((WIN, H), 0)
    far = 1 << 14

    def start_of(t):
        return pl.multiple_of((near_ref[HALF * t, 0] >> 4) << 4, 16)

    def windows_of(t):
        return ((near_ref[HALF * t + HALF - 1, H - 1] - start_of(t)) >> 6) + 1

    def mid_of(w):
        return pl.multiple_of((w >> 7) * STRIDE + ((w & 127) >> 4) * 24, 8)

    def rows_of(t):
        return pl.ds(pl.multiple_of(t * TILE, TILE), TILE)

    def lines(t):
        return [code_ref[pl.ds(HALF * t + k, 1), :] for k in range(HALF)]

    def columns(t):
        parts = [jnp.broadcast_to(line, (H, H)).T for line in lines(t)]
        return jnp.concatenate(parts, axis=0)

    def split(code, w, guard):
        place = code >> 11
        home = (code & 2047) - w
        if guard:
            place = jnp.where(jnp.logical_and(home >= 0, home < WIN), place, far)
        return place, home

    def gather_pre(col, w, rest, weights, guard):
        place, home = split(col, w, guard)
        mid = mid_of(w)
        left = [
            hot(place - mid == lane),
            hot(place - w == lane_x),
            hot(home == lane_self),
        ]
        right = [
            mid_ref[pl.ds(mid, MID), :].astype(BF16),
            ppad_ref[pl.ds(w + 2 * PLANE, WIN), :],
            ppad_ref[pl.ds(w, WIN), :],
            home_ref[pl.ds(w, MID), :],
        ]
        return dot(jnp.concatenate(left + rest, axis=1), jnp.concatenate(right + weights, axis=0))

    def activate(t, z):
        s = sigmoid(z)
        u = z * s
        ub = u.astype(BF16)
        u_ref[rows_of(t), :] = ub
        slope_ref[rows_of(t), :] = (s + u * (1.0 - s)).astype(BF16)
        return ub

    def collect(t, w, eu):
        ones = jnp.concatenate(
            [jnp.where((line & 2047) - w == wrow, 1.0, 0.0) for line in lines(t)], axis=1
        )
        eu_ref[pl.ds(w, WIN), :] += dot(ones.astype(BF16), eu)
        deg_ref[pl.ds(w, WIN), :] += jnp.broadcast_to(
            jnp.sum(ones, axis=1, keepdims=True), (WIN, H)
        )

    def forward_fast(t):
        col = columns(t)
        col_ref[rows_of(t), :] = col
        e = e_ref[rows_of(t), :]
        w = start_of(t)
        ub = activate(t, gather_pre(col, w, [e], [w1a], False))
        collect(t, w, jnp.concatenate([e, ub], axis=1))

    def forward_slow(t):
        col_ref[rows_of(t), :] = columns(t)
        zacc_ref[:, 0:H] = dot(e_ref[rows_of(t), :], w1a)

        def more(k, carry):
            w = pl.multiple_of(start_of(t) + k * WIN, 16)
            zacc_ref[:, 0:H] += gather_pre(col_ref[rows_of(t), :], w, [], [], True)
            return carry

        lax.fori_loop(0, windows_of(t), more, 0)
        activate(t, zacc_ref[:, 0:H])

        def put(k, carry):
            w = pl.multiple_of(start_of(t) + k * WIN, 16)
            collect(t, w, jnp.concatenate([e_ref[rows_of(t), :], u_ref[rows_of(t), :]], axis=1))
            return carry

        lax.fori_loop(0, windows_of(t), put, 0)

    def each_group(fast, slow, after=None):
        def body(g, carry):
            tiles = [g * GROUP + k for k in range(GROUP)]
            fits = windows_of(tiles[0]) <= 1
            for t in tiles[1:]:
                fits = jnp.logical_and(fits, windows_of(t) <= 1)

            @pl.when(fits)
            def _():
                for t in tiles:
                    fast(t)

            @pl.when(jnp.logical_not(fits))
            def _():
                for t in tiles:
                    slow(t)

            if after is not None:
                after(g)
            return carry

        lax.fori_loop(0, TILES // GROUP, body, 0)

    each_group(forward_fast, forward_slow)

    w2n_flip = flip(w2n_ref[...])
    w1n_flip = jnp.concatenate([flip(w1n_ref[0:H]), flip(w1n_ref[H : 2 * H])], axis=1)

    def cells(k, carry):
        at = pl.ds(pl.multiple_of(k * TILE, TILE), TILE)
        eu = eu_ref[at, :]
        usum = eu[:, H:]
        uh = usum.astype(BF16)
        ul = (usum - uh.astype(F32)).astype(BF16)
        w2 = w2e_ref[...]
        agg = (eu[:, 0:H] + deg_ref[at, :] * b2e_ref[...]) + dot(
            jnp.concatenate([uh, ul], axis=1), jnp.concatenate([w2, w2], axis=0)
        )
        x = jnp.concatenate([node_ref[at, :], agg.astype(BF16)], axis=1)
        z = dot(x, w1n_ref[...]) + b1n_ref[...]
        s = sigmoid(z)
        u = z * s
        cot = cotn_ref[at, :]
        dz = (dot(cot, w2n_flip) * (s + u * (1.0 - s))).astype(BF16)
        dx = dot(dz, w1n_flip)
        cot32 = cot.astype(F32)
        gown_ref[at, :] = cot32 + dx[:, 0:H]
        dagg = dx[:, H:].astype(BF16)
        dd_ref[at, 0:H] = dot(dagg, const_ref[:, 0:H]).astype(BF16)
        dd_ref[at, H:] = dagg
        par_ref[4 * H : 6 * H, :] += dot_first(x, dz)
        par_ref[6 * H : 7 * H, :] += dot_first(u.astype(BF16), cot)
        par_ref[7 * H + 2 : 7 * H + 3, :] += jnp.sum(dz.astype(F32), axis=0, keepdims=True)
        par_ref[7 * H + 3 : 7 * H + 4, :] += jnp.sum(cot32, axis=0, keepdims=True)
        return carry

    lax.fori_loop(0, CELLS // TILE, cells, 0, unroll=2)
    copy_cot.wait()

    def spread(col, w, cot):
        left = jnp.concatenate([hot((col & 2047) - w == lane), cot], axis=1)
        right = jnp.concatenate([dd_ref[pl.ds(w, H), :], const_ref[...]], axis=0)
        return dot(left, right)

    def scatter(t, w, dz, guard):
        mid = mid_of(w)
        parts = []
        for line in lines(t):
            place, home = split(line, w, guard)
            across = place - w
            parts.append(
                jnp.concatenate(
                    [
                        hot(place - mid == mrow),
                        hot(across - 4096 == wrow),
                        hot(across - 8192 == wrow),
                        hot(home == wrow),
                    ],
                    axis=0,
                )
            )
        sums = dot(jnp.concatenate(parts, axis=1), dz)
        smid_ref[pl.ds(mid, MID), :] += sums[0:MID]
        spad_ref[pl.ds(w + 2 * PLANE, WIN), :] += sums[MID : MID + WIN]
        spad_ref[pl.ds(w, WIN), :] += sums[MID + WIN : MID + 2 * WIN]
        rsum_ref[pl.ds(w, WIN), :] += sums[MID + 2 * WIN :]

    def finish_edges(t, dd):
        d32 = dd[:, H:]
        d = d32.astype(BF16)
        dz = (dd[:, 0:H] * slope_ref[rows_of(t), :].astype(F32)).astype(BF16)
        gedge_ref[rows_of(t), :] = (d32 + dot(dz, flip_ref[2 * H : 3 * H])).astype(BF16)
        wide_ref[0:H, :] += dot_first(e_ref[rows_of(t), :], dz)
        wide_ref[H : 2 * H, :] += dot_first(u_ref[rows_of(t), :], d)
        wide_ref[2 * H : 2 * H + 8, :] += jnp.sum(d32.reshape(TILE // 8, 8, H), axis=0)
        return dz

    def backward_fast(t):
        w = start_of(t)
        dz = finish_edges(t, spread(col_ref[rows_of(t), :], w, cot_ref[rows_of(t), :]))
        scatter(t, w, dz, False)

    def backward_slow(t):
        zacc_ref[...] = dot(cot_ref[rows_of(t), :], const_ref[...])

        def more(k, carry):
            w = pl.multiple_of(start_of(t) + k * H, 16)
            zacc_ref[...] += spread(
                col_ref[rows_of(t), :], w, jnp.zeros((TILE, H), BF16)
            )
            return carry

        lax.fori_loop(0, (windows_of(t) + 1) >> 1, more, 0)
        dz_ref[...] = finish_edges(t, zacc_ref[...])

        def put(k, carry):
            scatter(t, pl.multiple_of(start_of(t) + k * WIN, 16), dz_ref[...], True)
            return carry

        lax.fori_loop(0, windows_of(t), put, 0)

    per_chunk = TILES // GROUP // CHUNKS

    def send_out(g):
        @pl.when(g % per_chunk == per_chunk - 1)
        def _():
            copy_out(g // per_chunk).start()

    each_group(backward_fast, backward_slow, send_out)

    for i in range(N_PLANE):
        at = slice(i * PLANE, (i + 1) * PLANE)
        base = i * STRIDE
        for l in range(4):
            own_ref[pl.ds(i * PLANE + l, 32, 4), :] = smid_ref[pl.ds(base + 7 + l, 32, 6), :]
        zx_ref[0, i * 32 : (i + 1) * 32, :] = smid_ref[pl.ds(base + 6, 32, 6), :]
        zx_ref[1, i * 32 : (i + 1) * 32, :] = smid_ref[pl.ds(base + 11, 32, 6), :]
        nothing = jnp.zeros((4, H), F32)
        yx_ref[i * 8 : i * 8 + 8, :] = jnp.concatenate(
            [nothing, smid_ref[base + 1 : base + 5, :]], axis=0
        )
        yx_ref[PLANE + i * 8 : PLANE + i * 8 + 8, :] = jnp.concatenate(
            [smid_ref[base + 199 : base + 203, :], nothing], axis=0
        )

    def gather_cells(i, carry):
        base = pl.multiple_of(i * TILE, TILE)
        at = pl.ds(base, TILE)
        total = spad_ref[pl.ds(base + PLANE, TILE), :] + own_ref[at, :]
        sums = rsum_ref[at, :]
        par_ref[7 * H : 7 * H + 1, :] += jnp.sum(sums, axis=0, keepdims=True)
        sr16 = jnp.concatenate([total, sums], axis=1).astype(BF16)
        sr_ref[at, :] = sr16
        gown_ref[at, :] += dot(sr16, flip_ref[0 : 2 * H])
        return carry

    lax.fori_loop(0, CELLS // TILE, gather_cells, 0, unroll=2)
    both = dot_first(node_ref[...], sr_ref[...])
    w1b_flip = flip_ref[0:H]
    sx_lo = spad_ref[0:PLANE].astype(BF16)
    sx_hi = spad_ref[CELLS + PLANE : CELLS + 2 * PLANE].astype(BF16)
    sy_lo = yx_ref[0:PLANE].astype(BF16)
    sy_hi = yx_ref[PLANE : 2 * PLANE].astype(BF16)
    sz_lo = zx_ref[0].astype(BF16)
    sz_hi = zx_ref[1].astype(BF16)
    fx_ref[0] = dot(sx_lo, w1b_flip).astype(BF16)
    fx_ref[1] = dot(sx_hi, w1b_flip).astype(BF16)
    fy_ref[0] = dot(sy_lo, w1b_flip).astype(BF16)
    fy_ref[1] = dot(sy_hi, w1b_flip).astype(BF16)
    fz_ref[0] = dot(sz_lo, w1b_flip).astype(BF16)
    fz_ref[1] = dot(sz_hi, w1b_flip).astype(BF16)
    halo_x = dot_first(xlo_ref[...], sx_lo) + dot_first(xhi_ref[...], sx_hi)
    halo_y = dot_first(ylo_ref[...], sy_lo) + dot_first(yhi_ref[...], sy_hi)
    halo_z = dot_first(zlo_ref[...], sz_lo) + dot_first(zhi_ref[...], sz_hi)
    par_ref[0:H, :] = wide_ref[0:H, :]
    par_ref[H : 2 * H, :] = both[:, 0:H] + halo_x + halo_y + halo_z
    par_ref[2 * H : 3 * H, :] = both[:, H:]
    par_ref[3 * H : 4 * H, :] = wide_ref[H : 2 * H, :]
    par_ref[7 * H + 1 : 7 * H + 2, :] = jnp.sum(
        wide_ref[2 * H : 2 * H + 8, :], axis=0, keepdims=True
    )
    for c in range(CHUNKS):
        copy_out(c).wait()


def layer_call(senders, receivers, *arrays):
    smem = pl.BlockSpec(memory_space=pltpu.SMEM)
    vmem = pl.BlockSpec(memory_space=pltpu.VMEM)
    hbm = pl.BlockSpec(memory_space=pl.ANY)
    senders = senders.reshape(EDGES // H, H)
    receivers = receivers.reshape(EDGES // H, H)
    return pl.pallas_call(
        layer_kernel,
        in_specs=[smem] + [vmem] * 10 + [hbm] * 2 + [vmem] * 7,
        out_specs=[hbm] + [vmem] * 5,
        out_shape=[
            jax.ShapeDtypeStruct((EDGES, H), BF16),
            jax.ShapeDtypeStruct((CELLS, H), F32),
            jax.ShapeDtypeStruct((2, PLANE, H), BF16),
            jax.ShapeDtypeStruct((2, PLANE, H), BF16),
            jax.ShapeDtypeStruct((2, CELLS // 4, H), BF16),
            jax.ShapeDtypeStruct((PARAM_ROWS, H), F32),
        ],
        scratch_shapes=[
            pltpu.VMEM((EDGES, H), BF16),
            pltpu.VMEM((EDGES, H), BF16),
            pltpu.VMEM((EDGES, H), BF16),
            pltpu.VMEM((TILE, H), BF16),
            pltpu.VMEM((CELLS, H), F32),
            pltpu.VMEM((2, CELLS // 4, H), F32),
            pltpu.VMEM((2 * PLANE, H), F32),
            pltpu.VMEM((PAD_ROWS, H), BF16),
            pltpu.VMEM((ROWS, H), BF16),
            pltpu.VMEM((GRID, H), F32),
            pltpu.VMEM((EDGES // H, H), jnp.int32),
            pltpu.VMEM((EDGES, H), jnp.int32),
            pltpu.VMEM((EDGES, H), BF16),
            pltpu.VMEM((EDGES, H), BF16),
            pltpu.VMEM((ROWS, 2 * H), F32),
            pltpu.VMEM((ROWS, H), F32),
            pltpu.VMEM((ROWS, 2 * H), BF16),
            pltpu.VMEM((PAD_ROWS, H), F32),
            pltpu.VMEM((ROWS, H), F32),
            pltpu.VMEM((GRID, H), F32),
            pltpu.VMEM((2 * H + 8, H), F32),
            pltpu.VMEM((TILE, 2 * H), F32),
            pltpu.VMEM((H, 2 * H), BF16),
            pltpu.VMEM((3 * H, H), BF16),
            pltpu.VMEM((CELLS, 2 * H), BF16),
            pltpu.SemaphoreType.DMA((2,)),
            pltpu.SemaphoreType.DMA((CHUNKS,)),
        ],
        compiler_params=pltpu.CompilerParams(vmem_limit_bytes=60 * 1024 * 1024),
        name="layer",
    )(receivers, senders, receivers, *arrays)


def finish_kernel(
    gown_ref,
    xlo_ref,
    xhi_ref,
    ylo_ref,
    yhi_ref,
    zlo_ref,
    zhi_ref,
    par_ref,
    gnode_ref,
    w1e_ref,
    w2e_ref,
    w1n_ref,
    w2n_ref,
    bias_ref,
    sum_ref,
):
    par = par_ref[0 : 7 * H + 8, :]
    square = jnp.sum(par * par)
    factor = 1.0 / jnp.maximum(1.0, jnp.sqrt(jnp.full((1, H), square / (7 * H * H + 4 * H), F32)))
    w1e_ref[...] = par_ref[0 : 3 * H, :] * factor
    w2e_ref[...] = par_ref[3 * H : 4 * H, :] * factor
    w1n_ref[...] = par_ref[4 * H : 6 * H, :] * factor
    w2n_ref[...] = par_ref[6 * H : 7 * H, :] * factor
    bias_ref[...] = par_ref[7 * H : 7 * H + 4, :] * factor
    sum_ref[...] = gown_ref[...]
    sum_ref[0:PLANE] += xlo_ref[...].astype(F32)
    sum_ref[CELLS - PLANE :] += xhi_ref[...].astype(F32)
    for i in range(N_PLANE):
        low = ylo_ref[i * 8 : i * 8 + 8, :].astype(F32)
        high = yhi_ref[i * 8 : i * 8 + 8, :].astype(F32)
        sum_ref[i * PLANE : i * PLANE + 8, :] += low
        sum_ref[(i + 1) * PLANE - 8 : (i + 1) * PLANE, :] += high
    sum_ref[pl.ds(0, CELLS // 4, 4), :] += zlo_ref[...].astype(F32)
    sum_ref[pl.ds(3, CELLS // 4, 4), :] += zhi_ref[...].astype(F32)
    gnode_ref[...] = sum_ref[...].astype(BF16)


def finish_call(*arrays):
    return pl.pallas_call(
        finish_kernel,
        in_specs=[pl.BlockSpec(memory_space=pltpu.VMEM)] * 8,
        out_specs=[pl.BlockSpec(memory_space=pltpu.VMEM)] * 6,
        out_shape=[
            jax.ShapeDtypeStruct((CELLS, H), BF16),
            jax.ShapeDtypeStruct((3 * H, H), F32),
            jax.ShapeDtypeStruct((H, H), F32),
            jax.ShapeDtypeStruct((2 * H, H), F32),
            jax.ShapeDtypeStruct((H, H), F32),
            jax.ShapeDtypeStruct((4, H), F32),
        ],
        scratch_shapes=[pltpu.VMEM((CELLS, H), F32)],
        name="finish",
    )(*arrays)


def from_previous(value, axis):
    n = lax.axis_size(axis)
    return lax.ppermute(value, axis, [(k, (k + 1) % n) for k in range(n)])


def from_next(value, axis):
    n = lax.axis_size(axis)
    return lax.ppermute(value, axis, [((k + 1) % n, k) for k in range(n)])


def sum_over_devices(rows):
    count = 1
    for axis in AXES:
        count *= lax.axis_size(axis)
    chunks = rows.reshape(count, -1, H)
    mine = jnp.sum(lax.all_to_all(chunks, AXES, 0, 0, tiled=True), axis=0)
    copies = jnp.broadcast_to(mine[None], (count,) + mine.shape)
    return lax.all_to_all(copies, AXES, 0, 0, tiled=True).reshape(-1, H)


def on_device(
    node_latent,
    edge_latent,
    senders,
    receivers,
    w1_edge,
    b1_edge,
    w2_edge,
    b2_edge,
    w1_node,
    b1_node,
    w2_node,
    cot_node,
    cot_edge,
):
    zlo = from_previous(node_latent[:, :, 3], "gz").reshape(-1, H)
    zhi = from_next(node_latent[:, :, 0], "gz").reshape(-1, H)
    ylo = from_previous(node_latent[:, 30:32], "gy").reshape(-1, H)
    yhi = from_next(node_latent[:, 0:2], "gy").reshape(-1, H)
    xlo = from_previous(node_latent[15], "gx").reshape(-1, H)
    xhi = from_next(node_latent[0], "gx").reshape(-1, H)
    gedge, gown, fx, fy, fz, par = layer_call(
        senders,
        receivers,
        node_latent.reshape(CELLS, H),
        cot_node.reshape(CELLS, H),
        xlo,
        xhi,
        ylo,
        yhi,
        zlo,
        zhi,
        edge_latent.reshape(EDGES, H),
        cot_edge.reshape(EDGES, H),
        w1_edge,
        b1_edge.reshape(1, H),
        w2_edge,
        b2_edge.reshape(1, H),
        w1_node,
        b1_node.reshape(1, H),
        w2_node,
    )
    full = sum_over_devices(par)
    gnode, gw1e, gw2e, gw1n, gw2n, gbias = finish_call(
        gown,
        from_previous(fx[1], "gx"),
        from_next(fx[0], "gx"),
        from_previous(fy[1], "gy"),
        from_next(fy[0], "gy"),
        from_previous(fz[1], "gz"),
        from_next(fz[0], "gz"),
        full,
    )
    return (
        gnode.reshape(node_latent.shape),
        gedge.reshape(edge_latent.shape),
        gw1e,
        gw2e,
        gw1n,
        gw2n,
        gbias,
    )


def solution(mesh):
    cells = P("gx", "gy", "gz", None)
    edges = P("gx", "gy", "gz", None, None)
    return jax.shard_map(
        on_device,
        mesh=mesh,
        in_specs=(cells, edges, cells, cells) + (P(),) * 7 + (cells, edges),
        out_specs=(cells, edges) + (P(),) * 5,
        check_vma=False,
    )
```

```python
import jax
import jax.numpy as jnp
from jax import lax
from jax.experimental import pallas as pl
from jax.experimental.pallas import tpu as pltpu
from jax.sharding import PartitionSpec as P

H = 128
PLANE = 128
N_PLANE = 16
CELLS = N_PLANE * PLANE
EDGES = 12288
TILE = 256
TILES = EDGES // TILE
WIN = 64
MID = 128
GROUP = 8
HALF = TILE // H
CHUNKS = 3
ROWS = CELLS + 128
STRIDE = 208
GRID = N_PLANE * STRIDE + 128
PAD_ROWS = CELLS + 3 * PLANE
PARAM_ROWS = 1024
AXES = ("gx", "gy", "gz")
F32 = jnp.float32
BF16 = jnp.bfloat16


def dot(a, b):
    return lax.dot_general(a, b, (((1,), (0,)), ((), ())), preferred_element_type=F32)


def dot_first(a, b):
    return lax.dot_general(a, b, (((0,), (0,)), ((), ())), preferred_element_type=F32)


def flip(w):
    return w.astype(F32).T.astype(BF16)


def hot(mask):
    return jnp.where(mask, 1.0, 0.0).astype(BF16)


def iota(shape, dim):
    return lax.broadcasted_iota(jnp.int32, shape, dim)


def sigmoid(v):
    return 0.5 * jnp.tanh(0.5 * v) + 0.5


def layer_kernel(
    near_ref,
    send_ref,
    recv_ref,
    node_ref,
    cotn_ref,
    xlo_ref,
    xhi_ref,
    ylo_ref,
    yhi_ref,
    zlo_ref,
    zhi_ref,
    e_hbm,
    cot_hbm,
    w1e_ref,
    b1e_ref,
    w2e_ref,
    b2e_ref,
    w1n_ref,
    b1n_ref,
    w2n_ref,
    gedge_hbm,
    gown_ref,
    fx_ref,
    fy_ref,
    fz_ref,
    par_ref,
    e_ref,
    cot_ref,
    gedge_ref,
    dz_ref,
    own_ref,
    zx_ref,
    yx_ref,
    ppad_ref,
    home_ref,
    mid_ref,
    code_ref,
    col_ref,
    u_ref,
    slope_ref,
    eu_ref,
    deg_ref,
    dd_ref,
    spad_ref,
    rsum_ref,
    smid_ref,
    wide_ref,
    zacc_ref,
    const_ref,
    flip_ref,
    sr_ref,
    in_sem,
    out_sem,
):
    copy_e = pltpu.make_async_copy(e_hbm, e_ref, in_sem.at[0])
    copy_cot = pltpu.make_async_copy(cot_hbm, cot_ref, in_sem.at[1])
    copy_e.start()
    copy_cot.start()

    def copy_out(c):
        size = EDGES // CHUNKS
        at = pl.ds(pl.multiple_of(c * size, size), size)
        return pltpu.make_async_copy(gedge_ref.at[at, :], gedge_hbm.at[at, :], out_sem.at[c])

    w1a = w1e_ref[0:H]
    w1b = w1e_ref[H : 2 * H]
    w1c = w1e_ref[2 * H : 3 * H]
    par_ref[...] = jnp.zeros(par_ref.shape, F32)
    eu_ref[...] = jnp.zeros(eu_ref.shape, F32)
    deg_ref[...] = jnp.zeros(deg_ref.shape, F32)
    spad_ref[...] = jnp.zeros(spad_ref.shape, F32)
    rsum_ref[...] = jnp.zeros(rsum_ref.shape, F32)
    smid_ref[...] = jnp.zeros(smid_ref.shape, F32)
    mid_ref[...] = jnp.zeros(mid_ref.shape, F32)
    wide_ref[...] = jnp.zeros(wide_ref.shape, F32)
    dd_ref[CELLS:ROWS] = jnp.zeros((ROWS - CELLS, 2 * H), F32)
    home_ref[CELLS:ROWS] = jnp.zeros((ROWS - CELLS, H), F32)
    ppad_ref[CELLS + 2 * PLANE :] = jnp.zeros((PAD_ROWS - CELLS - 2 * PLANE, H), F32)
    const_ref[:, 0:H] = flip(w2e_ref[...])
    const_ref[:, H:] = hot(iota((H, H), 0) == iota((H, H), 1))
    flip_ref[0:H] = flip(w1b)
    flip_ref[H : 2 * H] = flip(w1c)
    flip_ref[2 * H : 3 * H] = flip(w1a)

    r = recv_ref[...]
    s = send_ref[...]
    delta = s - (((r >> 7) + 1) * 204 + (((r >> 2) & 31) + 1) * 6 + (r & 3) + 1)
    inside = s - 204 + 4 * (r >> 7)
    place = jnp.where(delta == 204, r + 4096, jnp.where(delta == -204, r + 8192, inside))
    code_ref[...] = place * 2048 + r

    ppad_ref[0:PLANE] = dot(xlo_ref[...], w1b)
    ppad_ref[CELLS + PLANE : CELLS + 2 * PLANE] = dot(xhi_ref[...], w1b)
    yx_ref[0:PLANE] = dot(ylo_ref[...], w1b)
    yx_ref[PLANE : 2 * PLANE] = dot(yhi_ref[...], w1b)
    zx_ref[0] = dot(zlo_ref[...], w1b)
    zx_ref[1] = dot(zhi_ref[...], w1b)
    own_ref[...] = dot(node_ref[...], w1b)
    for i in range(N_PLANE):
        at = slice(i * PLANE, (i + 1) * PLANE)
        base = i * STRIDE
        ppad_ref[(i + 1) * PLANE : (i + 2) * PLANE] = own_ref[at]
        home_ref[at] = dot(node_ref[at], w1c) + b1e_ref[...]
        for l in range(4):
            mid_ref[pl.ds(base + 7 + l, 32, 6), :] = own_ref[pl.ds(i * PLANE + l, 32, 4), :]
        mid_ref[pl.ds(base + 6, 32, 6), :] = zx_ref[0, i * 32 : (i + 1) * 32, :]
        mid_ref[pl.ds(base + 11, 32, 6), :] = zx_ref[1, i * 32 : (i + 1) * 32, :]
        mid_ref[base + 1 : base + 5, :] = yx_ref[i * 8 + 4 : i * 8 + 8, :]
        mid_ref[base + 199 : base + 203, :] = yx_ref[PLANE + i * 8 : PLANE + i * 8 + 4, :]
    copy_e.wait()

    lane = iota((TILE, H), 1)
    lane_x = jnp.where(lane < WIN, 4096 + lane, 8192 - WIN + lane)
    lane_self = jnp.where(lane < WIN, lane, -(1 << 20))
    mrow = iota((MID, H), 0)
    wrow = iota((WIN, H), 0)
    far = 1 << 14

    def start_of(t):
        return pl.multiple_of((near_ref[HALF * t, 0] >> 3) << 3, 8)

    def windows_of(t):
        return ((near_ref[HALF * t + HALF - 1, H - 1] - start_of(t)) >> 6) + 1

    def mid_of(w):
        return pl.multiple_of((w >> 7) * STRIDE + ((w & 127) >> 4) * 24 + (w & 8), 8)

    def rows_of(t):
        return pl.ds(pl.multiple_of(t * TILE, TILE), TILE)

    def lines(t):
        return [code_ref[pl.ds(HALF * t + k, 1), :] for k in range(HALF)]

    def columns(t):
        parts = [jnp.broadcast_to(line, (H, H)).T for line in lines(t)]
        return jnp.concatenate(parts, axis=0)

    def split(code, w, guard):
        place = code >> 11
        home = (code & 2047) - w
        if guard:
            place = jnp.where(jnp.logical_and(home >= 0, home < WIN), place, far)
        return place, home

    def gather_pre(col, w, rest, weights, guard):
        place, home = split(col, w, guard)
        mid = mid_of(w)
        left = [
            hot(place - mid == lane),
            hot(place - w == lane_x),
            hot(home == lane_self),
        ]
        right = [
            mid_ref[pl.ds(mid, MID), :].astype(BF16),
            ppad_ref[pl.ds(w + 2 * PLANE, WIN), :].astype(BF16),
            ppad_ref[pl.ds(w, WIN), :].astype(BF16),
            home_ref[pl.ds(w, MID), :].astype(BF16),
        ]
        return dot(jnp.concatenate(left + rest, axis=1), jnp.concatenate(right + weights, axis=0))

    def activate(t, z):
        s = sigmoid(z)
        u = z * s
        ub = u.astype(BF16)
        u_ref[rows_of(t), :] = ub
        slope_ref[rows_of(t), :] = (s + u * (1.0 - s)).astype(BF16)
        return ub

    def collect(t, w, eu):
        ones = jnp.concatenate(
            [jnp.where((line & 2047) - w == wrow, 1.0, 0.0) for line in lines(t)], axis=1
        )
        eu_ref[pl.ds(w, WIN), :] += dot(ones.astype(BF16), eu)
        deg_ref[pl.ds(w, WIN), :] += jnp.broadcast_to(
            jnp.sum(ones, axis=1, keepdims=True), (WIN, H)
        )

    def forward_fast(t):
        col = columns(t)
        col_ref[rows_of(t), :] = col
        e = e_ref[rows_of(t), :]
        w = start_of(t)
        ub = activate(t, gather_pre(col, w, [e], [w1a], False))
        collect(t, w, jnp.concatenate([e, ub], axis=1))

    def forward_slow(t):
        col_ref[rows_of(t), :] = columns(t)
        zacc_ref[:, 0:H] = dot(e_ref[rows_of(t), :], w1a)

        def more(k, carry):
            w = pl.multiple_of(start_of(t) + k * WIN, 8)
            zacc_ref[:, 0:H] += gather_pre(col_ref[rows_of(t), :], w, [], [], True)
            return carry

        lax.fori_loop(0, windows_of(t), more, 0)
        activate(t, zacc_ref[:, 0:H])

        def put(k, carry):
            w = pl.multiple_of(start_of(t) + k * WIN, 8)
            collect(t, w, jnp.concatenate([e_ref[rows_of(t), :], u_ref[rows_of(t), :]], axis=1))
            return carry

        lax.fori_loop(0, windows_of(t), put, 0)

    def each_group(fast, slow, after=None):
        def body(g, carry):
            tiles = [g * GROUP + k for k in range(GROUP)]
            fits = windows_of(tiles[0]) <= 1
            for t in tiles[1:]:
                fits = jnp.logical_and(fits, windows_of(t) <= 1)

            @pl.when(fits)
            def _():
                for t in tiles:
                    fast(t)

            @pl.when(jnp.logical_not(fits))
            def _():
                for t in tiles:
                    slow(t)

            if after is not None:
                after(g)
            return carry

        lax.fori_loop(0, TILES // GROUP, body, 0)

    each_group(forward_fast, forward_slow)

    w2n_flip = flip(w2n_ref[...])
    w1n_flip = jnp.concatenate([flip(w1n_ref[0:H]), flip(w1n_ref[H : 2 * H])], axis=1)

    def cells(k, carry):
        at = pl.ds(pl.multiple_of(k * TILE, TILE), TILE)
        eu = eu_ref[at, :]
        usum = eu[:, H:]
        uh = usum.astype(BF16)
        ul = (usum - uh.astype(F32)).astype(BF16)
        w2 = w2e_ref[...]
        agg = (eu[:, 0:H] + deg_ref[at, :] * b2e_ref[...]) + dot(
            jnp.concatenate([uh, ul], axis=1), jnp.concatenate([w2, w2], axis=0)
        )
        x = jnp.concatenate([node_ref[at, :], agg.astype(BF16)], axis=1)
        z = dot(x, w1n_ref[...]) + b1n_ref[...]
        s = sigmoid(z)
        u = z * s
        cot = cotn_ref[at, :]
        dz = (dot(cot, w2n_flip) * (s + u * (1.0 - s))).astype(BF16)
        dx = dot(dz, w1n_flip)
        cot32 = cot.astype(F32)
        gown_ref[at, :] = cot32 + dx[:, 0:H]
        dagg = dx[:, H:].astype(BF16)
        dd_ref[at, 0:H] = dot(dagg, const_ref[:, 0:H])
        dd_ref[at, H:] = dx[:, H:]
        par_ref[4 * H : 6 * H, :] += dot_first(x, dz)
        par_ref[6 * H : 7 * H, :] += dot_first(u.astype(BF16), cot)
        par_ref[7 * H + 2 : 7 * H + 3, :] += jnp.sum(dz.astype(F32), axis=0, keepdims=True)
        par_ref[7 * H + 3 : 7 * H + 4, :] += jnp.sum(cot32, axis=0, keepdims=True)
        return carry

    lax.fori_loop(0, CELLS // TILE, cells, 0, unroll=8)
    copy_cot.wait()

    def spread(col, w, cot):
        left = jnp.concatenate([hot((col & 2047) - w == lane), cot], axis=1)
        right = jnp.concatenate([dd_ref[pl.ds(w, H), :].astype(BF16), const_ref[...]], axis=0)
        return dot(left, right)

    def scatter(t, w, dz, guard):
        mid = mid_of(w)
        parts = []
        for line in lines(t):
            place, home = split(line, w, guard)
            across = place - w
            parts.append(
                jnp.concatenate(
                    [
                        hot(place - mid == mrow),
                        hot(across - 4096 == wrow),
                        hot(across - 8192 == wrow),
                        hot(home == wrow),
                    ],
                    axis=0,
                )
            )
        sums = dot(jnp.concatenate(parts, axis=1), dz)
        smid_ref[pl.ds(mid, MID), :] += sums[0:MID]
        spad_ref[pl.ds(w + 2 * PLANE, WIN), :] += sums[MID : MID + WIN]
        spad_ref[pl.ds(w, WIN), :] += sums[MID + WIN : MID + 2 * WIN]
        rsum_ref[pl.ds(w, WIN), :] += sums[MID + 2 * WIN :]

    def finish_edges(t, dd):
        d32 = dd[:, H:]
        d = d32.astype(BF16)
        dz = (dd[:, 0:H] * slope_ref[rows_of(t), :].astype(F32)).astype(BF16)
        gedge_ref[rows_of(t), :] = (d32 + dot(dz, flip_ref[2 * H : 3 * H])).astype(BF16)
        wide_ref[0:H, :] += dot_first(e_ref[rows_of(t), :], dz)
        wide_ref[H : 2 * H, :] += dot_first(u_ref[rows_of(t), :], d)
        wide_ref[2 * H : 2 * H + 8, :] += jnp.sum(d32.reshape(TILE // 8, 8, H), axis=0)
        return dz

    def backward_fast(t):
        w = start_of(t)
        dz = finish_edges(t, spread(col_ref[rows_of(t), :], w, cot_ref[rows_of(t), :]))
        scatter(t, w, dz, False)

    def backward_slow(t):
        zacc_ref[...] = dot(cot_ref[rows_of(t), :], const_ref[...])

        def more(k, carry):
            w = pl.multiple_of(start_of(t) + k * H, 8)
            zacc_ref[...] += spread(
                col_ref[rows_of(t), :], w, jnp.zeros((TILE, H), BF16)
            )
            return carry

        lax.fori_loop(0, (windows_of(t) + 1) >> 1, more, 0)
        dz_ref[...] = finish_edges(t, zacc_ref[...])

        def put(k, carry):
            scatter(t, pl.multiple_of(start_of(t) + k * WIN, 8), dz_ref[...], True)
            return carry

        lax.fori_loop(0, windows_of(t), put, 0)

    per_chunk = TILES // GROUP // CHUNKS

    def send_out(g):
        @pl.when(g % per_chunk == per_chunk - 1)
        def _():
            copy_out(g // per_chunk).start()

    each_group(backward_fast, backward_slow, send_out)

    for i in range(N_PLANE):
        at = slice(i * PLANE, (i + 1) * PLANE)
        base = i * STRIDE
        for l in range(4):
            own_ref[pl.ds(i * PLANE + l, 32, 4), :] = smid_ref[pl.ds(base + 7 + l, 32, 6), :]
        zx_ref[0, i * 32 : (i + 1) * 32, :] = smid_ref[pl.ds(base + 6, 32, 6), :]
        zx_ref[1, i * 32 : (i + 1) * 32, :] = smid_ref[pl.ds(base + 11, 32, 6), :]
        nothing = jnp.zeros((4, H), F32)
        yx_ref[i * 8 : i * 8 + 8, :] = jnp.concatenate(
            [nothing, smid_ref[base + 1 : base + 5, :]], axis=0
        )
        yx_ref[PLANE + i * 8 : PLANE + i * 8 + 8, :] = jnp.concatenate(
            [smid_ref[base + 199 : base + 203, :], nothing], axis=0
        )

    def gather_cells(i, carry):
        base = pl.multiple_of(i * TILE, TILE)
        at = pl.ds(base, TILE)
        total = spad_ref[pl.ds(base + PLANE, TILE), :] + own_ref[at, :]
        sums = rsum_ref[at, :]
        par_ref[7 * H : 7 * H + 1, :] += jnp.sum(sums, axis=0, keepdims=True)
        sr16 = jnp.concatenate([total, sums], axis=1).astype(BF16)
        sr_ref[at, :] = sr16
        gown_ref[at, :] += dot(sr16, flip_ref[0 : 2 * H])
        return carry

    lax.fori_loop(0, CELLS // TILE, gather_cells, 0, unroll=8)
    both = dot_first(node_ref[...], sr_ref[...])
    w1b_flip = flip_ref[0:H]
    sx_lo = spad_ref[0:PLANE].astype(BF16)
    sx_hi = spad_ref[CELLS + PLANE : CELLS + 2 * PLANE].astype(BF16)
    sy_lo = yx_ref[0:PLANE].astype(BF16)
    sy_hi = yx_ref[PLANE : 2 * PLANE].astype(BF16)
    sz_lo = zx_ref[0].astype(BF16)
    sz_hi = zx_ref[1].astype(BF16)
    fx_ref[0] = dot(sx_lo, w1b_flip).astype(BF16)
    fx_ref[1] = dot(sx_hi, w1b_flip).astype(BF16)
    fy_ref[0] = dot(sy_lo, w1b_flip).astype(BF16)
    fy_ref[1] = dot(sy_hi, w1b_flip).astype(BF16)
    fz_ref[0] = dot(sz_lo, w1b_flip).astype(BF16)
    fz_ref[1] = dot(sz_hi, w1b_flip).astype(BF16)
    halo_x = dot_first(xlo_ref[...], sx_lo) + dot_first(xhi_ref[...], sx_hi)
    halo_y = dot_first(ylo_ref[...], sy_lo) + dot_first(yhi_ref[...], sy_hi)
    halo_z = dot_first(zlo_ref[...], sz_lo) + dot_first(zhi_ref[...], sz_hi)
    par_ref[0:H, :] = wide_ref[0:H, :]
    par_ref[H : 2 * H, :] = both[:, 0:H] + halo_x + halo_y + halo_z
    par_ref[2 * H : 3 * H, :] = both[:, H:]
    par_ref[3 * H : 4 * H, :] = wide_ref[H : 2 * H, :]
    par_ref[7 * H + 1 : 7 * H + 2, :] = jnp.sum(
        wide_ref[2 * H : 2 * H + 8, :], axis=0, keepdims=True
    )
    for c in range(CHUNKS):
        copy_out(c).wait()


def layer_call(senders, receivers, *arrays):
    smem = pl.BlockSpec(memory_space=pltpu.SMEM)
    vmem = pl.BlockSpec(memory_space=pltpu.VMEM)
    hbm = pl.BlockSpec(memory_space=pl.ANY)
    senders = senders.reshape(EDGES // H, H)
    receivers = receivers.reshape(EDGES // H, H)
    return pl.pallas_call(
        layer_kernel,
        in_specs=[smem] + [vmem] * 10 + [hbm] * 2 + [vmem] * 7,
        out_specs=[hbm] + [vmem] * 5,
        out_shape=[
            jax.ShapeDtypeStruct((EDGES, H), BF16),
            jax.ShapeDtypeStruct((CELLS, H), F32),
            jax.ShapeDtypeStruct((2, PLANE, H), BF16),
            jax.ShapeDtypeStruct((2, PLANE, H), BF16),
            jax.ShapeDtypeStruct((2, CELLS // 4, H), BF16),
            jax.ShapeDtypeStruct((PARAM_ROWS, H), F32),
        ],
        scratch_shapes=[
            pltpu.VMEM((EDGES, H), BF16),
            pltpu.VMEM((EDGES, H), BF16),
            pltpu.VMEM((EDGES, H), BF16),
            pltpu.VMEM((TILE, H), BF16),
            pltpu.VMEM((CELLS, H), F32),
            pltpu.VMEM((2, CELLS // 4, H), F32),
            pltpu.VMEM((2 * PLANE, H), F32),
            pltpu.VMEM((PAD_ROWS, H), F32),
            pltpu.VMEM((ROWS, H), F32),
            pltpu.VMEM((GRID, H), F32),
            pltpu.VMEM((EDGES // H, H), jnp.int32),
            pltpu.VMEM((EDGES, H), jnp.int32),
            pltpu.VMEM((EDGES, H), BF16),
            pltpu.VMEM((EDGES, H), BF16),
            pltpu.VMEM((ROWS, 2 * H), F32),
            pltpu.VMEM((ROWS, H), F32),
            pltpu.VMEM((ROWS, 2 * H), F32),
            pltpu.VMEM((PAD_ROWS, H), F32),
            pltpu.VMEM((ROWS, H), F32),
            pltpu.VMEM((GRID, H), F32),
            pltpu.VMEM((2 * H + 8, H), F32),
            pltpu.VMEM((TILE, 2 * H), F32),
            pltpu.VMEM((H, 2 * H), BF16),
            pltpu.VMEM((3 * H, H), BF16),
            pltpu.VMEM((CELLS, 2 * H), BF16),
            pltpu.SemaphoreType.DMA((2,)),
            pltpu.SemaphoreType.DMA((CHUNKS,)),
        ],
        compiler_params=pltpu.CompilerParams(vmem_limit_bytes=60 * 1024 * 1024),
        name="layer",
    )(receivers, senders, receivers, *arrays)


def finish_kernel(
    gown_ref,
    xlo_ref,
    xhi_ref,
    ylo_ref,
    yhi_ref,
    zlo_ref,
    zhi_ref,
    par_ref,
    gnode_ref,
    w1e_ref,
    w2e_ref,
    w1n_ref,
    w2n_ref,
    bias_ref,
    sum_ref,
):
    par = par_ref[0 : 7 * H + 8, :]
    square = jnp.sum(par * par)
    factor = 1.0 / jnp.maximum(1.0, jnp.sqrt(jnp.full((1, H), square / (7 * H * H + 4 * H), F32)))
    w1e_ref[...] = par_ref[0 : 3 * H, :] * factor
    w2e_ref[...] = par_ref[3 * H : 4 * H, :] * factor
    w1n_ref[...] = par_ref[4 * H : 6 * H, :] * factor
    w2n_ref[...] = par_ref[6 * H : 7 * H, :] * factor
    bias_ref[...] = par_ref[7 * H : 7 * H + 4, :] * factor
    sum_ref[...] = gown_ref[...]
    sum_ref[0:PLANE] += xlo_ref[...].astype(F32)
    sum_ref[CELLS - PLANE :] += xhi_ref[...].astype(F32)
    for i in range(N_PLANE):
        low = ylo_ref[i * 8 : i * 8 + 8, :].astype(F32)
        high = yhi_ref[i * 8 : i * 8 + 8, :].astype(F32)
        sum_ref[i * PLANE : i * PLANE + 8, :] += low
        sum_ref[(i + 1) * PLANE - 8 : (i + 1) * PLANE, :] += high
    sum_ref[pl.ds(0, CELLS // 4, 4), :] += zlo_ref[...].astype(F32)
    sum_ref[pl.ds(3, CELLS // 4, 4), :] += zhi_ref[...].astype(F32)
    gnode_ref[...] = sum_ref[...].astype(BF16)


def finish_call(*arrays):
    return pl.pallas_call(
        finish_kernel,
        in_specs=[pl.BlockSpec(memory_space=pltpu.VMEM)] * 8,
        out_specs=[pl.BlockSpec(memory_space=pltpu.VMEM)] * 6,
        out_shape=[
            jax.ShapeDtypeStruct((CELLS, H), BF16),
            jax.ShapeDtypeStruct((3 * H, H), F32),
            jax.ShapeDtypeStruct((H, H), F32),
            jax.ShapeDtypeStruct((2 * H, H), F32),
            jax.ShapeDtypeStruct((H, H), F32),
            jax.ShapeDtypeStruct((4, H), F32),
        ],
        scratch_shapes=[pltpu.VMEM((CELLS, H), F32)],
        name="finish",
    )(*arrays)


def from_previous(value, axis):
    n = lax.axis_size(axis)
    return lax.ppermute(value, axis, [(k, (k + 1) % n) for k in range(n)])


def from_next(value, axis):
    n = lax.axis_size(axis)
    return lax.ppermute(value, axis, [((k + 1) % n, k) for k in range(n)])


def sum_over_devices(rows):
    count = 1
    for axis in AXES:
        count *= lax.axis_size(axis)
    chunks = rows.reshape(count, -1, H)
    mine = jnp.sum(lax.all_to_all(chunks, AXES, 0, 0, tiled=True), axis=0)
    copies = jnp.broadcast_to(mine[None], (count,) + mine.shape)
    return lax.all_to_all(copies, AXES, 0, 0, tiled=True).reshape(-1, H)


def on_device(
    node_latent,
    edge_latent,
    senders,
    receivers,
    w1_edge,
    b1_edge,
    w2_edge,
    b2_edge,
    w1_node,
    b1_node,
    w2_node,
    cot_node,
    cot_edge,
):
    zlo = from_previous(node_latent[:, :, 3], "gz").reshape(-1, H)
    zhi = from_next(node_latent[:, :, 0], "gz").reshape(-1, H)
    ylo = from_previous(node_latent[:, 30:32], "gy").reshape(-1, H)
    yhi = from_next(node_latent[:, 0:2], "gy").reshape(-1, H)
    xlo = from_previous(node_latent[15], "gx").reshape(-1, H)
    xhi = from_next(node_latent[0], "gx").reshape(-1, H)
    gedge, gown, fx, fy, fz, par = layer_call(
        senders,
        receivers,
        node_latent.reshape(CELLS, H),
        cot_node.reshape(CELLS, H),
        xlo,
        xhi,
        ylo,
        yhi,
        zlo,
        zhi,
        edge_latent.reshape(EDGES, H),
        cot_edge.reshape(EDGES, H),
        w1_edge,
        b1_edge.reshape(1, H),
        w2_edge,
        b2_edge.reshape(1, H),
        w1_node,
        b1_node.reshape(1, H),
        w2_node,
    )
    full = sum_over_devices(par)
    gnode, gw1e, gw2e, gw1n, gw2n, gbias = finish_call(
        gown,
        from_previous(fx[1], "gx"),
        from_next(fx[0], "gx"),
        from_previous(fy[1], "gy"),
        from_next(fy[0], "gy"),
        from_previous(fz[1], "gz"),
        from_next(fz[0], "gz"),
        full,
    )
    return (
        gnode.reshape(node_latent.shape),
        gedge.reshape(edge_latent.shape),
        gw1e,
        gw2e,
        gw1n,
        gw2n,
        gbias,
    )


def solution(mesh):
    cells = P("gx", "gy", "gz", None)
    edges = P("gx", "gy", "gz", None, None)
    return jax.shard_map(
        on_device,
        mesh=mesh,
        in_specs=(cells, edges, cells, cells) + (P(),) * 7 + (cells, edges),
        out_specs=(cells, edges) + (P(),) * 5,
        check_vma=False,
    )
```

```python
import jax
import jax.numpy as jnp
from jax import lax
from jax.experimental import pallas as pl
from jax.experimental.pallas import tpu as pltpu
from jax.sharding import PartitionSpec as P


H = 128
PLANE = 128
N_PLANE = 16
CELLS = N_PLANE * PLANE
EDGES = 12288
TILE = 256
TILES = EDGES // TILE
WIN = 64
MID = 128
GROUP = 8
HALF = TILE // H
CHUNKS = 3
ROWS = CELLS + 128
STRIDE = 208
GRID = N_PLANE * STRIDE + 128
PAD_ROWS = CELLS + 3 * PLANE
PARAM_ROWS = 1024
AXES = ("gx", "gy", "gz")
F32 = jnp.float32
BF16 = jnp.bfloat16


def dot(a, b):
    return lax.dot_general(a, b, (((1,), (0,)), ((), ())), preferred_element_type=F32)


def dot_first(a, b):
    return lax.dot_general(a, b, (((0,), (0,)), ((), ())), preferred_element_type=F32)


def flip(w):
    return w.astype(F32).T.astype(BF16)


def hot(mask):
    return jnp.where(mask, 1.0, 0.0).astype(BF16)


def iota(shape, dim):
    return lax.broadcasted_iota(jnp.int32, shape, dim)


def sigmoid(v):
    return 0.5 * jnp.tanh(0.5 * v) + 0.5


def layer_kernel(
    near_ref,
    send_ref,
    recv_ref,
    node_ref,
    cotn_ref,
    xlo_ref,
    xhi_ref,
    ylo_ref,
    yhi_ref,
    zlo_ref,
    zhi_ref,
    e_hbm,
    cot_hbm,
    w1e_ref,
    b1e_ref,
    w2e_ref,
    b2e_ref,
    w1n_ref,
    b1n_ref,
    w2n_ref,
    gedge_hbm,
    gown_ref,
    fx_ref,
    fy_ref,
    fz_ref,
    par_out,
    e_ref,
    cot_ref,
    gedge_ref,
    dz_ref,
    own_ref,
    zx_ref,
    yx_ref,
    ppad_ref,
    home_ref,
    mid_ref,
    place_ref,
    col_ref,
    u_ref,
    slope_ref,
    eu_ref,
    deg_ref,
    dd_ref,
    spad_ref,
    rsum_ref,
    smid_ref,
    wide_ref,
    zacc_ref,
    const_ref,
    flip_ref,
    sr_ref,
    par_ref,
    in_sem,
    out_sem,
):
    copy_e = pltpu.make_async_copy(e_hbm, e_ref, in_sem.at[0])
    copy_cot = pltpu.make_async_copy(cot_hbm, cot_ref, in_sem.at[1])
    copy_e.start()
    copy_cot.start()

    def copy_out(c):
        size = EDGES // CHUNKS
        at = pl.ds(pl.multiple_of(c * size, size), size)
        return pltpu.make_async_copy(gedge_ref.at[at, :], gedge_hbm.at[at, :], out_sem.at[c])

    w1a = w1e_ref[0:H]
    w1b = w1e_ref[H : 2 * H]
    w1c = w1e_ref[2 * H : 3 * H]
    w1a_half = (0.5 * w1a.astype(F32)).astype(BF16)
    w1b_half = (0.5 * w1b.astype(F32)).astype(BF16)
    w1c_half = (0.5 * w1c.astype(F32)).astype(BF16)
    par_ref[...] = jnp.zeros(par_ref.shape, F32)
    eu_ref[...] = jnp.zeros(eu_ref.shape, F32)
    deg_ref[...] = jnp.zeros(deg_ref.shape, F32)
    spad_ref[...] = jnp.zeros(spad_ref.shape, F32)
    rsum_ref[...] = jnp.zeros(rsum_ref.shape, F32)
    smid_ref[...] = jnp.zeros(smid_ref.shape, F32)
    mid_ref[...] = jnp.zeros(mid_ref.shape, F32)
    wide_ref[...] = jnp.zeros(wide_ref.shape, F32)
    dd_ref[CELLS:ROWS] = jnp.zeros((ROWS - CELLS, 2 * H), F32)
    home_ref[CELLS:ROWS] = jnp.zeros((ROWS - CELLS, H), F32)
    ppad_ref[CELLS + 2 * PLANE :] = jnp.zeros((PAD_ROWS - CELLS - 2 * PLANE, H), F32)
    w2_half = (0.5 * w2e_ref[...].astype(F32)).astype(BF16)
    const_ref[:, 0:H] = flip(w2_half)
    const_ref[:, H:] = hot(iota((H, H), 0) == iota((H, H), 1))
    flip_ref[0:H] = flip(w1b)
    flip_ref[H : 2 * H] = flip(w1c)
    flip_ref[2 * H : 3 * H] = flip(w1a)

    r = recv_ref[...]
    s = send_ref[...]
    delta = s - (((r >> 7) + 1) * 204 + (((r >> 2) & 31) + 1) * 6 + (r & 3) + 1)
    inside = s - 204 + 4 * (r >> 7)
    place = jnp.where(delta == 204, r + 4096, jnp.where(delta == -204, r + 8192, inside))
    place_ref[...] = place

    ppad_ref[0:PLANE] = dot(xlo_ref[...], w1b_half)
    ppad_ref[CELLS + PLANE : CELLS + 2 * PLANE] = dot(xhi_ref[...], w1b_half)
    yx_ref[0:PLANE] = dot(ylo_ref[...], w1b_half)
    yx_ref[PLANE : 2 * PLANE] = dot(yhi_ref[...], w1b_half)
    zx_ref[0] = dot(zlo_ref[...], w1b_half)
    zx_ref[1] = dot(zhi_ref[...], w1b_half)
    own_ref[...] = dot(node_ref[...], w1b_half)
    for i in range(N_PLANE):
        at = slice(i * PLANE, (i + 1) * PLANE)
        base = i * STRIDE
        ppad_ref[(i + 1) * PLANE : (i + 2) * PLANE] = own_ref[at]
        home_ref[at] = dot(node_ref[at], w1c_half) + 0.5 * b1e_ref[...]
        for l in range(4):
            mid_ref[pl.ds(base + 7 + l, 32, 6), :] = own_ref[pl.ds(i * PLANE + l, 32, 4), :]
        mid_ref[pl.ds(base + 6, 32, 6), :] = zx_ref[0, i * 32 : (i + 1) * 32, :]
        mid_ref[pl.ds(base + 11, 32, 6), :] = zx_ref[1, i * 32 : (i + 1) * 32, :]
        mid_ref[base + 1 : base + 5, :] = yx_ref[i * 8 + 4 : i * 8 + 8, :]
        mid_ref[base + 199 : base + 203, :] = yx_ref[PLANE + i * 8 : PLANE + i * 8 + 4, :]
    copy_e.wait()

    lane = iota((TILE, H), 1)
    lane_x = jnp.where(lane < WIN, 4096 + lane, 8192 - WIN + lane)
    lane_self = jnp.where(lane < WIN, lane, -(1 << 20))
    mrow = iota((MID, H), 0)
    wrow = iota((WIN, H), 0)
    far = 1 << 14

    def start_of(t):
        return pl.multiple_of((near_ref[HALF * t, 0] >> 3) << 3, 8)

    def windows_of(t):
        return ((near_ref[HALF * t + HALF - 1, H - 1] - start_of(t)) >> 6) + 1

    def mid_of(w):
        return pl.multiple_of((w >> 7) * STRIDE + ((w & 127) >> 4) * 24 + (w & 8), 8)

    def rows_of(t):
        return pl.ds(pl.multiple_of(t * TILE, TILE), TILE)

    def places(t):
        return [place_ref[pl.ds(HALF * t + k, 1), :] for k in range(HALF)]

    def homes(t):
        return [recv_ref[pl.ds(HALF * t + k, 1), :] for k in range(HALF)]

    def columns(lines):
        return jnp.concatenate([jnp.broadcast_to(line, (H, H)).T for line in lines], axis=0)

    def keep_near(place, home, w):
        return jnp.where(jnp.logical_and(home >= w, home < w + WIN), place, far)

    def gather_pre(place, home, w, rest, weights):
        mid = mid_of(w)
        left = [
            hot(place == lane + mid),
            hot(place == lane_x + w),
            hot(home == lane_self + w),
        ]
        right = [
            mid_ref[pl.ds(mid, MID), :].astype(BF16),
            ppad_ref[pl.ds(w + 2 * PLANE, WIN), :].astype(BF16),
            ppad_ref[pl.ds(w, WIN), :].astype(BF16),
            home_ref[pl.ds(w, MID), :].astype(BF16),
        ]
        return dot(jnp.concatenate(left + rest, axis=1), jnp.concatenate(right + weights, axis=0))

    def activate(t, half):
        th = jnp.tanh(half)
        up = 1.0 + th
        u = half * up
        ub = u.astype(BF16)
        u_ref[rows_of(t), :] = ub
        slope_ref[rows_of(t), :] = (up + u * (1.0 - th)).astype(BF16)
        return ub

    def collect(t, w, eu):
        ones = jnp.concatenate(
            [jnp.where(line == wrow + w, 1.0, 0.0) for line in homes(t)], axis=1
        )
        eu_ref[pl.ds(w, WIN), :] += dot(ones.astype(BF16), eu)
        deg_ref[pl.ds(w, WIN), :] += jnp.broadcast_to(
            jnp.sum(ones, axis=1, keepdims=True), (WIN, H)
        )

    def forward_fast(t):
        home = columns(homes(t))
        col_ref[rows_of(t), :] = home
        e = e_ref[rows_of(t), :]
        w = start_of(t)
        ub = activate(t, gather_pre(columns(places(t)), home, w, [e], [w1a_half]))
        collect(t, w, jnp.concatenate([e, ub], axis=1))

    def forward_slow(t):
        col_ref[rows_of(t), :] = columns(homes(t))
        zacc_ref[:, 0:H] = dot(e_ref[rows_of(t), :], w1a_half)

        def more(k, carry):
            w = pl.multiple_of(start_of(t) + k * WIN, 8)
            home = col_ref[rows_of(t), :]
            place = keep_near(columns(places(t)), home, w)
            zacc_ref[:, 0:H] += gather_pre(place, home, w, [], [])
            return carry

        lax.fori_loop(0, windows_of(t), more, 0)
        activate(t, zacc_ref[:, 0:H])

        def put(k, carry):
            w = pl.multiple_of(start_of(t) + k * WIN, 8)
            collect(t, w, jnp.concatenate([e_ref[rows_of(t), :], u_ref[rows_of(t), :]], axis=1))
            return carry

        lax.fori_loop(0, windows_of(t), put, 0)

    def each_group(fast, slow, after=None):
        def body(g, carry):
            tiles = [g * GROUP + k for k in range(GROUP)]
            fits = windows_of(tiles[0]) <= 1
            for t in tiles[1:]:
                fits = jnp.logical_and(fits, windows_of(t) <= 1)

            @pl.when(fits)
            def _():
                for t in tiles:
                    fast(t)

            @pl.when(jnp.logical_not(fits))
            def _():
                for t in tiles:
                    slow(t)

            if after is not None:
                after(g)
            return carry

        lax.fori_loop(0, TILES // GROUP, body, 0)

    each_group(forward_fast, forward_slow)

    w2n_flip = flip(w2n_ref[...])
    w1n_flip = jnp.concatenate([flip(w1n_ref[0:H]), flip(w1n_ref[H : 2 * H])], axis=1)

    def cells(k, carry):
        at = pl.ds(pl.multiple_of(k * TILE, TILE), TILE)
        eu = eu_ref[at, :]
        usum = eu[:, H:]
        uh = usum.astype(BF16)
        ul = (usum - uh.astype(F32)).astype(BF16)
        w2 = w2e_ref[...]
        agg = (eu[:, 0:H] + deg_ref[at, :] * b2e_ref[...]) + dot(
            jnp.concatenate([uh, ul], axis=1), jnp.concatenate([w2, w2], axis=0)
        )
        x = jnp.concatenate([node_ref[at, :], agg.astype(BF16)], axis=1)
        z = dot(x, w1n_ref[...]) + b1n_ref[...]
        s = sigmoid(z)
        u = z * s
        cot = cotn_ref[at, :]
        dz = (dot(cot, w2n_flip) * (s + u * (1.0 - s))).astype(BF16)
        dx = dot(dz, w1n_flip)
        cot32 = cot.astype(F32)
        gown_ref[at, :] = cot32 + dx[:, 0:H]
        dagg = dx[:, H:].astype(BF16)
        dd_ref[at, 0:H] = dot(dagg, const_ref[:, 0:H])
        dd_ref[at, H:] = dx[:, H:]
        par_ref[4 * H : 6 * H, :] += dot_first(x, dz)
        par_ref[6 * H : 7 * H, :] += dot_first(u.astype(BF16), cot)
        par_ref[7 * H + 2 : 7 * H + 3, :] += jnp.sum(dz.astype(F32), axis=0, keepdims=True)
        par_ref[7 * H + 3 : 7 * H + 4, :] += jnp.sum(cot32, axis=0, keepdims=True)
        return carry

    lax.fori_loop(0, CELLS // TILE, cells, 0, unroll=8)
    copy_cot.wait()

    def spread(home, w, cot):
        left = jnp.concatenate([hot(home == lane + w), cot], axis=1)
        right = jnp.concatenate([dd_ref[pl.ds(w, H), :].astype(BF16), const_ref[...]], axis=0)
        return dot(left, right)

    def scatter(t, w, dz, guard):
        mid = mid_of(w)
        parts = []
        for place, home in zip(places(t), homes(t)):
            if guard:
                place = keep_near(place, home, w)
            parts.append(
                jnp.concatenate(
                    [
                        hot(place == mrow + mid),
                        hot(place == wrow + (w + 4096)),
                        hot(place == wrow + (w + 8192)),
                        hot(home == wrow + w),
                    ],
                    axis=0,
                )
            )
        sums = dot(jnp.concatenate(parts, axis=1), dz)
        smid_ref[pl.ds(mid, MID), :] += sums[0:MID]
        spad_ref[pl.ds(w + 2 * PLANE, WIN), :] += sums[MID : MID + WIN]
        spad_ref[pl.ds(w, WIN), :] += sums[MID + WIN : MID + 2 * WIN]
        rsum_ref[pl.ds(w, WIN), :] += sums[MID + 2 * WIN :]

    def finish_edges(t, dd):
        d32 = dd[:, H:]
        d = d32.astype(BF16)
        dz = (dd[:, 0:H] * slope_ref[rows_of(t), :].astype(F32)).astype(BF16)
        gedge_ref[rows_of(t), :] = (d32 + dot(dz, flip_ref[2 * H : 3 * H])).astype(BF16)
        wide_ref[0:H, :] += dot_first(e_ref[rows_of(t), :], dz)
        wide_ref[H : 2 * H, :] += dot_first(u_ref[rows_of(t), :], d)
        wide_ref[2 * H : 2 * H + 8, :] += jnp.sum(d32.reshape(TILE // 8, 8, H), axis=0)
        return dz

    def backward_fast(t):
        w = start_of(t)
        dz = finish_edges(t, spread(col_ref[rows_of(t), :], w, cot_ref[rows_of(t), :]))
        scatter(t, w, dz, False)

    def backward_slow(t):
        zacc_ref[...] = dot(cot_ref[rows_of(t), :], const_ref[...])

        def more(k, carry):
            w = pl.multiple_of(start_of(t) + k * H, 8)
            zacc_ref[...] += spread(
                col_ref[rows_of(t), :], w, jnp.zeros((TILE, H), BF16)
            )
            return carry

        lax.fori_loop(0, (windows_of(t) + 1) >> 1, more, 0)
        dz_ref[...] = finish_edges(t, zacc_ref[...])

        def put(k, carry):
            scatter(t, pl.multiple_of(start_of(t) + k * WIN, 8), dz_ref[...], True)
            return carry

        lax.fori_loop(0, windows_of(t), put, 0)

    per_chunk = TILES // GROUP // CHUNKS

    def send_out(g):
        @pl.when(g % per_chunk == per_chunk - 1)
        def _():
            copy_out(g // per_chunk).start()

    each_group(backward_fast, backward_slow, send_out)

    for i in range(N_PLANE):
        at = slice(i * PLANE, (i + 1) * PLANE)
        base = i * STRIDE
        for l in range(4):
            own_ref[pl.ds(i * PLANE + l, 32, 4), :] = smid_ref[pl.ds(base + 7 + l, 32, 6), :]
        zx_ref[0, i * 32 : (i + 1) * 32, :] = smid_ref[pl.ds(base + 6, 32, 6), :]
        zx_ref[1, i * 32 : (i + 1) * 32, :] = smid_ref[pl.ds(base + 11, 32, 6), :]
        nothing = jnp.zeros((4, H), F32)
        yx_ref[i * 8 : i * 8 + 8, :] = jnp.concatenate(
            [nothing, smid_ref[base + 1 : base + 5, :]], axis=0
        )
        yx_ref[PLANE + i * 8 : PLANE + i * 8 + 8, :] = jnp.concatenate(
            [smid_ref[base + 199 : base + 203, :], nothing], axis=0
        )

    def gather_cells(i, carry):
        base = pl.multiple_of(i * TILE, TILE)
        at = pl.ds(base, TILE)
        total = spad_ref[pl.ds(base + PLANE, TILE), :] + own_ref[at, :]
        sums = rsum_ref[at, :]
        par_ref[7 * H : 7 * H + 1, :] += jnp.sum(sums, axis=0, keepdims=True)
        sr16 = jnp.concatenate([total, sums], axis=1).astype(BF16)
        sr_ref[at, :] = sr16
        gown_ref[at, :] += dot(sr16, flip_ref[0 : 2 * H])
        return carry

    lax.fori_loop(0, CELLS // TILE, gather_cells, 0, unroll=8)
    both = dot_first(node_ref[...], sr_ref[...])
    w1b_flip = flip_ref[0:H]
    sx_lo = spad_ref[0:PLANE].astype(BF16)
    sx_hi = spad_ref[CELLS + PLANE : CELLS + 2 * PLANE].astype(BF16)
    sy_lo = yx_ref[0:PLANE].astype(BF16)
    sy_hi = yx_ref[PLANE : 2 * PLANE].astype(BF16)
    sz_lo = zx_ref[0].astype(BF16)
    sz_hi = zx_ref[1].astype(BF16)
    fx_ref[0] = dot(sx_lo, w1b_flip).astype(BF16)
    fx_ref[1] = dot(sx_hi, w1b_flip).astype(BF16)
    fy_ref[0] = dot(sy_lo, w1b_flip).astype(BF16)
    fy_ref[1] = dot(sy_hi, w1b_flip).astype(BF16)
    fz_ref[0] = dot(sz_lo, w1b_flip).astype(BF16)
    fz_ref[1] = dot(sz_hi, w1b_flip).astype(BF16)
    halo_x = dot_first(xlo_ref[...], sx_lo) + dot_first(xhi_ref[...], sx_hi)
    halo_y = dot_first(ylo_ref[...], sy_lo) + dot_first(yhi_ref[...], sy_hi)
    halo_z = dot_first(zlo_ref[...], sz_lo) + dot_first(zhi_ref[...], sz_hi)
    par_ref[0:H, :] = wide_ref[0:H, :]
    par_ref[H : 2 * H, :] = both[:, 0:H] + halo_x + halo_y + halo_z
    par_ref[2 * H : 3 * H, :] = both[:, H:]
    par_ref[3 * H : 4 * H, :] = wide_ref[H : 2 * H, :]
    par_ref[7 * H + 1 : 7 * H + 2, :] = jnp.sum(
        wide_ref[2 * H : 2 * H + 8, :], axis=0, keepdims=True
    )
    par_out[...] = par_ref[...].astype(BF16)
    for c in range(CHUNKS):
        copy_out(c).wait()


def layer_call(senders, receivers, *arrays):
    smem = pl.BlockSpec(memory_space=pltpu.SMEM)
    vmem = pl.BlockSpec(memory_space=pltpu.VMEM)
    hbm = pl.BlockSpec(memory_space=pl.ANY)
    senders = senders.reshape(EDGES // H, H)
    receivers = receivers.reshape(EDGES // H, H)
    return pl.pallas_call(
        layer_kernel,
        in_specs=[smem] + [vmem] * 10 + [hbm] * 2 + [vmem] * 7,
        out_specs=[hbm] + [vmem] * 5,
        out_shape=[
            jax.ShapeDtypeStruct((EDGES, H), BF16),
            jax.ShapeDtypeStruct((CELLS, H), F32),
            jax.ShapeDtypeStruct((2, PLANE, H), BF16),
            jax.ShapeDtypeStruct((2, PLANE, H), BF16),
            jax.ShapeDtypeStruct((2, CELLS // 4, H), BF16),
            jax.ShapeDtypeStruct((PARAM_ROWS, H), BF16),
        ],
        scratch_shapes=[
            pltpu.VMEM((EDGES, H), BF16),
            pltpu.VMEM((EDGES, H), BF16),
            pltpu.VMEM((EDGES, H), BF16),
            pltpu.VMEM((TILE, H), BF16),
            pltpu.VMEM((CELLS, H), F32),
            pltpu.VMEM((2, CELLS // 4, H), F32),
            pltpu.VMEM((2 * PLANE, H), F32),
            pltpu.VMEM((PAD_ROWS, H), F32),
            pltpu.VMEM((ROWS, H), F32),
            pltpu.VMEM((GRID, H), F32),
            pltpu.VMEM((EDGES // H, H), jnp.int32),
            pltpu.VMEM((EDGES, H), jnp.int32),
            pltpu.VMEM((EDGES, H), BF16),
            pltpu.VMEM((EDGES, H), BF16),
            pltpu.VMEM((ROWS, 2 * H), F32),
            pltpu.VMEM((ROWS, H), F32),
            pltpu.VMEM((ROWS, 2 * H), F32),
            pltpu.VMEM((PAD_ROWS, H), F32),
            pltpu.VMEM((ROWS, H), F32),
            pltpu.VMEM((GRID, H), F32),
            pltpu.VMEM((2 * H + 8, H), F32),
            pltpu.VMEM((TILE, 2 * H), F32),
            pltpu.VMEM((H, 2 * H), BF16),
            pltpu.VMEM((3 * H, H), BF16),
            pltpu.VMEM((CELLS, 2 * H), BF16),
            pltpu.VMEM((PARAM_ROWS, H), F32),
            pltpu.SemaphoreType.DMA((2,)),
            pltpu.SemaphoreType.DMA((CHUNKS,)),
        ],
        compiler_params=pltpu.CompilerParams(vmem_limit_bytes=60 * 1024 * 1024),
        name="layer",
    )(receivers, senders, receivers, *arrays)


def node_kernel(
    gown_ref,
    xlo_ref,
    xhi_ref,
    ylo_ref,
    yhi_ref,
    zlo_ref,
    zhi_ref,
    gnode_ref,
    sum_ref,
):
    sum_ref[...] = gown_ref[...]
    sum_ref[0:PLANE] += xlo_ref[...].astype(F32)
    sum_ref[CELLS - PLANE :] += xhi_ref[...].astype(F32)
    for i in range(N_PLANE):
        low = ylo_ref[i * 8 : i * 8 + 8, :].astype(F32)
        high = yhi_ref[i * 8 : i * 8 + 8, :].astype(F32)
        sum_ref[i * PLANE : i * PLANE + 8, :] += low
        sum_ref[(i + 1) * PLANE - 8 : (i + 1) * PLANE, :] += high
    sum_ref[pl.ds(0, CELLS // 4, 4), :] += zlo_ref[...].astype(F32)
    sum_ref[pl.ds(3, CELLS // 4, 4), :] += zhi_ref[...].astype(F32)
    gnode_ref[...] = sum_ref[...].astype(BF16)


def node_call(*arrays):
    return pl.pallas_call(
        node_kernel,
        in_specs=[pl.BlockSpec(memory_space=pltpu.VMEM)] * 7,
        out_specs=pl.BlockSpec(memory_space=pltpu.VMEM),
        out_shape=jax.ShapeDtypeStruct((CELLS, H), BF16),
        scratch_shapes=[pltpu.VMEM((CELLS, H), F32)],
        name="nodes",
    )(*arrays)


def clip_kernel(par_ref, w1e_ref, w2e_ref, w1n_ref, w2n_ref, bias_ref):
    par = par_ref[0 : 7 * H + 16, :].astype(F32)
    square = jnp.sum(par * par)
    factor = 1.0 / jnp.maximum(1.0, jnp.sqrt(jnp.full((1, H), square / (7 * H * H + 4 * H), F32)))
    w1e_ref[...] = par[0 : 3 * H] * factor
    w2e_ref[...] = par[3 * H : 4 * H] * factor
    w1n_ref[...] = par[4 * H : 6 * H] * factor
    w2n_ref[...] = par[6 * H : 7 * H] * factor
    bias_ref[...] = par[7 * H : 7 * H + 4] * factor


def clip_call(par):
    return pl.pallas_call(
        clip_kernel,
        in_specs=[pl.BlockSpec(memory_space=pltpu.VMEM)],
        out_specs=[pl.BlockSpec(memory_space=pltpu.VMEM)] * 5,
        out_shape=[
            jax.ShapeDtypeStruct((3 * H, H), F32),
            jax.ShapeDtypeStruct((H, H), F32),
            jax.ShapeDtypeStruct((2 * H, H), F32),
            jax.ShapeDtypeStruct((H, H), F32),
            jax.ShapeDtypeStruct((4, H), F32),
        ],
        name="clip",
    )(par)


def from_previous(value, axis):
    n = lax.axis_size(axis)
    return lax.ppermute(value, axis, [(k, (k + 1) % n) for k in range(n)])


def from_next(value, axis):
    n = lax.axis_size(axis)
    return lax.ppermute(value, axis, [((k + 1) % n, k) for k in range(n)])


def sum_over_devices(rows):
    count = 1
    for axis in AXES:
        count *= lax.axis_size(axis)
    chunks = rows.reshape(count, -1, H)
    parts = lax.all_to_all(chunks, AXES, 0, 0, tiled=True)
    mine = jnp.sum(parts.astype(F32), axis=0).astype(BF16)
    copies = jnp.broadcast_to(mine[None], (count,) + mine.shape)
    return lax.all_to_all(copies, AXES, 0, 0, tiled=True).reshape(-1, H)


def on_device(
    node_latent,
    edge_latent,
    senders,
    receivers,
    w1_edge,
    b1_edge,
    w2_edge,
    b2_edge,
    w1_node,
    b1_node,
    w2_node,
    cot_node,
    cot_edge,
):
    zlo = from_previous(node_latent[:, :, 3], "gz").reshape(-1, H)
    zhi = from_next(node_latent[:, :, 0], "gz").reshape(-1, H)
    ylo = from_previous(node_latent[:, 30:32], "gy").reshape(-1, H)
    yhi = from_next(node_latent[:, 0:2], "gy").reshape(-1, H)
    xlo = from_previous(node_latent[15], "gx").reshape(-1, H)
    xhi = from_next(node_latent[0], "gx").reshape(-1, H)
    gedge, gown, fx, fy, fz, par = layer_call(
        senders,
        receivers,
        node_latent.reshape(CELLS, H),
        cot_node.reshape(CELLS, H),
        xlo,
        xhi,
        ylo,
        yhi,
        zlo,
        zhi,
        edge_latent.reshape(EDGES, H),
        cot_edge.reshape(EDGES, H),
        w1_edge,
        b1_edge.reshape(1, H),
        w2_edge,
        b2_edge.reshape(1, H),
        w1_node,
        b1_node.reshape(1, H),
        w2_node,
    )
    full = sum_over_devices(par)
    gnode = node_call(
        gown,
        from_previous(fx[1], "gx"),
        from_next(fx[0], "gx"),
        from_previous(fy[1], "gy"),
        from_next(fy[0], "gy"),
        from_previous(fz[1], "gz"),
        from_next(fz[0], "gz"),
    )
    gw1e, gw2e, gw1n, gw2n, gbias = clip_call(full)
    return (
        gnode.reshape(node_latent.shape),
        gedge.reshape(edge_latent.shape),
        gw1e,
        gw2e,
        gw1n,
        gw2n,
        gbias,
    )


def solution(mesh):
    cells = P("gx", "gy", "gz", None)
    edges = P("gx", "gy", "gz", None, None)
    return jax.shard_map(
        on_device,
        mesh=mesh,
        in_specs=(cells, edges, cells, cells) + (P(),) * 7 + (cells, edges),
        out_specs=(cells, edges) + (P(),) * 5,
        check_vma=False,
    )
```

```python
import jax
import jax.numpy as jnp
from jax import lax
from jax.experimental import pallas as pl
from jax.experimental.pallas import tpu as pltpu
from jax.sharding import PartitionSpec as P


H = 128
PLANE = 128
N_PLANE = 16
CELLS = N_PLANE * PLANE
EDGES = 12288
TILE = 256
TILES = EDGES // TILE
WIN = 64
MID = 128
GROUP = 12
HALF = TILE // H
CHUNKS = 4
ROWS = CELLS + 128
STRIDE = 208
GRID = N_PLANE * STRIDE + 128
PAD_ROWS = CELLS + 3 * PLANE
PARAM_ROWS = 1024
AXES = ("gx", "gy", "gz")
F32 = jnp.float32
BF16 = jnp.bfloat16


def dot(a, b):
    return lax.dot_general(a, b, (((1,), (0,)), ((), ())), preferred_element_type=F32)


def dot_first(a, b):
    return lax.dot_general(a, b, (((0,), (0,)), ((), ())), preferred_element_type=F32)


def flip(w):
    return w.astype(F32).T.astype(BF16)


def hot(mask):
    return jnp.where(mask, 1.0, 0.0).astype(BF16)


def iota(shape, dim):
    return lax.broadcasted_iota(jnp.int32, shape, dim)


def sigmoid(v):
    return 0.5 * jnp.tanh(0.5 * v) + 0.5


def layer_kernel(
    near_ref,
    send_ref,
    recv_ref,
    node_ref,
    cotn_hbm,
    xlo_ref,
    xhi_ref,
    ylo_ref,
    yhi_ref,
    zlo_ref,
    zhi_ref,
    e_hbm,
    cot_hbm,
    w1e_ref,
    b1e_ref,
    w2e_ref,
    b2e_ref,
    w1n_ref,
    b1n_ref,
    w2n_ref,
    gedge_hbm,
    gown_ref,
    fxlo_ref,
    fxhi_ref,
    fylo_ref,
    fyhi_ref,
    fzlo_ref,
    fzhi_ref,
    par_out,
    e_ref,
    cot_ref,
    cotn_ref,
    gedge_ref,
    dz_ref,
    own_ref,
    zx_ref,
    yx_ref,
    ppad_ref,
    home_ref,
    mid_ref,
    place_ref,
    col_ref,
    u_ref,
    slope_ref,
    eu_ref,
    deg_ref,
    dd_ref,
    spad_ref,
    rsum_ref,
    smid_ref,
    wide_ref,
    zacc_ref,
    const_ref,
    flip_ref,
    sr_ref,
    par_ref,
    in_sem,
    out_sem,
):
    copy_e = pltpu.make_async_copy(e_hbm, e_ref, in_sem.at[0])
    copy_cot = pltpu.make_async_copy(cot_hbm, cot_ref, in_sem.at[1])
    copy_cotn = pltpu.make_async_copy(cotn_hbm, cotn_ref, in_sem.at[2])
    copy_e.start()
    copy_cotn.start()
    copy_cot.start()

    def copy_out(c):
        size = EDGES // CHUNKS
        at = pl.ds(pl.multiple_of(c * size, size), size)
        return pltpu.make_async_copy(gedge_ref.at[at, :], gedge_hbm.at[at, :], out_sem.at[c])

    w1a = w1e_ref[0:H]
    w1b = w1e_ref[H : 2 * H]
    w1c = w1e_ref[2 * H : 3 * H]
    w1a_half = (0.5 * w1a.astype(F32)).astype(BF16)
    w1b_half = (0.5 * w1b.astype(F32)).astype(BF16)
    w1c_half = (0.5 * w1c.astype(F32)).astype(BF16)
    par_ref[...] = jnp.zeros(par_ref.shape, F32)
    eu_ref[...] = jnp.zeros(eu_ref.shape, F32)
    deg_ref[...] = jnp.zeros(deg_ref.shape, F32)
    spad_ref[...] = jnp.zeros(spad_ref.shape, F32)
    rsum_ref[...] = jnp.zeros(rsum_ref.shape, F32)
    smid_ref[...] = jnp.zeros(smid_ref.shape, F32)
    mid_ref[N_PLANE * STRIDE :] = jnp.zeros((GRID - N_PLANE * STRIDE, H), F32)
    wide_ref[...] = jnp.zeros(wide_ref.shape, F32)
    dd_ref[CELLS:ROWS] = jnp.zeros((ROWS - CELLS, 2 * H), F32)
    home_ref[CELLS:ROWS] = jnp.zeros((ROWS - CELLS, H), F32)
    ppad_ref[CELLS + 2 * PLANE :] = jnp.zeros((PAD_ROWS - CELLS - 2 * PLANE, H), F32)
    w2_half = (0.5 * w2e_ref[...].astype(F32)).astype(BF16)
    const_ref[:, 0:H] = flip(w2_half)
    const_ref[:, H:] = hot(iota((H, H), 0) == iota((H, H), 1))
    flip_ref[0:H] = flip(w1b)
    flip_ref[H : 2 * H] = flip(w1c)
    flip_ref[2 * H : 3 * H] = flip(w1a)

    r = recv_ref[...]
    s = send_ref[...]
    delta = s - (((r >> 7) + 1) * 204 + (((r >> 2) & 31) + 1) * 6 + (r & 3) + 1)
    inside = s - 204 + 4 * (r >> 7)
    place = jnp.where(delta == 204, r + 4096, jnp.where(delta == -204, r + 8192, inside))
    place_ref[...] = place

    ppad_ref[0:PLANE] = dot(xlo_ref[...], w1b_half)
    ppad_ref[CELLS + PLANE : CELLS + 2 * PLANE] = dot(xhi_ref[...], w1b_half)
    yx_ref[0:PLANE] = dot(ylo_ref[...], w1b_half)
    yx_ref[PLANE : 2 * PLANE] = dot(yhi_ref[...], w1b_half)
    zx_ref[0] = dot(zlo_ref[...], w1b_half)
    zx_ref[1] = dot(zhi_ref[...], w1b_half)
    own_ref[...] = dot(node_ref[...], w1b_half)
    for i in range(N_PLANE):
        at = slice(i * PLANE, (i + 1) * PLANE)
        base = i * STRIDE
        ppad_ref[(i + 1) * PLANE : (i + 2) * PLANE] = own_ref[at]
        home_ref[at] = dot(node_ref[at], w1c_half) + 0.5 * b1e_ref[...]
        mid_ref[base : base + 8, :] = jnp.zeros((8, H), F32)
        mid_ref[base + 192 : base + 208, :] = jnp.zeros((16, H), F32)
        for l in range(4):
            mid_ref[pl.ds(base + 7 + l, 32, 6), :] = own_ref[pl.ds(i * PLANE + l, 32, 4), :]
        mid_ref[pl.ds(base + 6, 32, 6), :] = zx_ref[0, i * 32 : (i + 1) * 32, :]
        mid_ref[pl.ds(base + 11, 32, 6), :] = zx_ref[1, i * 32 : (i + 1) * 32, :]
        mid_ref[base + 1 : base + 5, :] = yx_ref[i * 8 + 4 : i * 8 + 8, :]
        mid_ref[base + 199 : base + 203, :] = yx_ref[PLANE + i * 8 : PLANE + i * 8 + 4, :]
    copy_e.wait()

    lane = iota((TILE, H), 1)
    lane_x = jnp.where(lane < WIN, 4096 + lane, 8192 - WIN + lane)
    lane_self = jnp.where(lane < WIN, lane, -(1 << 20))
    mrow = iota((MID, H), 0)
    wrow = iota((WIN, H), 0)
    far = 1 << 14

    def start_of(t):
        return pl.multiple_of((near_ref[HALF * t, 0] >> 3) << 3, 8)

    def windows_of(t):
        return ((near_ref[HALF * t + HALF - 1, H - 1] - start_of(t)) >> 6) + 1

    def mid_of(w):
        return pl.multiple_of((w >> 7) * STRIDE + ((w & 127) >> 4) * 24 + (w & 8), 8)

    def rows_of(t):
        return pl.ds(pl.multiple_of(t * TILE, TILE), TILE)

    def places(t):
        return [place_ref[pl.ds(HALF * t + k, 1), :] for k in range(HALF)]

    def homes(t):
        return [recv_ref[pl.ds(HALF * t + k, 1), :] for k in range(HALF)]

    def columns(lines):
        return jnp.concatenate([jnp.broadcast_to(line, (H, H)).T for line in lines], axis=0)

    def keep_near(place, home, w):
        return jnp.where(jnp.logical_and(home >= w, home < w + WIN), place, far)

    def gather_pre(place, home, w, rest, weights):
        mid = mid_of(w)
        left = [
            hot(place == lane + mid),
            hot(place == lane_x + w),
            hot(home == lane_self + w),
        ]
        right = [
            mid_ref[pl.ds(mid, MID), :].astype(BF16),
            ppad_ref[pl.ds(w + 2 * PLANE, WIN), :].astype(BF16),
            ppad_ref[pl.ds(w, WIN), :].astype(BF16),
            home_ref[pl.ds(w, MID), :].astype(BF16),
        ]
        return dot(jnp.concatenate(left + rest, axis=1), jnp.concatenate(right + weights, axis=0))

    def activate(t, half):
        th = jnp.tanh(half)
        up = 1.0 + th
        u = half * up
        ub = u.astype(BF16)
        u_ref[rows_of(t), :] = ub
        slope_ref[rows_of(t), :] = (up + u * (1.0 - th)).astype(BF16)
        return ub

    def collect(t, w, eu):
        ones = jnp.concatenate(
            [jnp.where(line == wrow + w, 1.0, 0.0) for line in homes(t)], axis=1
        )
        eu_ref[pl.ds(w, WIN), :] += dot(ones.astype(BF16), eu)
        deg_ref[pl.ds(w, WIN), :] += jnp.broadcast_to(
            jnp.sum(ones, axis=1, keepdims=True), (WIN, H)
        )

    def forward_fast(t):
        home = columns(homes(t))
        col_ref[rows_of(t), :] = home
        e = e_ref[rows_of(t), :]
        w = start_of(t)
        ub = activate(t, gather_pre(columns(places(t)), home, w, [e], [w1a_half]))
        collect(t, w, jnp.concatenate([e, ub], axis=1))

    def forward_slow(t):
        col_ref[rows_of(t), :] = columns(homes(t))
        zacc_ref[:, 0:H] = dot(e_ref[rows_of(t), :], w1a_half)

        def more(k, carry):
            w = pl.multiple_of(start_of(t) + k * WIN, 8)
            home = col_ref[rows_of(t), :]
            place = keep_near(columns(places(t)), home, w)
            zacc_ref[:, 0:H] += gather_pre(place, home, w, [], [])
            return carry

        lax.fori_loop(0, windows_of(t), more, 0)
        activate(t, zacc_ref[:, 0:H])

        def put(k, carry):
            w = pl.multiple_of(start_of(t) + k * WIN, 8)
            collect(t, w, jnp.concatenate([e_ref[rows_of(t), :], u_ref[rows_of(t), :]], axis=1))
            return carry

        lax.fori_loop(0, windows_of(t), put, 0)

    def each_group(fast, slow, after=None):
        def body(g, carry):
            tiles = [g * GROUP + k for k in range(GROUP)]
            fits = windows_of(tiles[0]) <= 1
            for t in tiles[1:]:
                fits = jnp.logical_and(fits, windows_of(t) <= 1)

            @pl.when(fits)
            def _():
                for t in tiles:
                    fast(t)

            @pl.when(jnp.logical_not(fits))
            def _():
                def one(k, inner):
                    slow(g * GROUP + k)
                    return inner

                lax.fori_loop(0, GROUP, one, 0)

            if after is not None:
                after(g)
            return carry

        lax.fori_loop(0, TILES // GROUP, body, 0)

    each_group(forward_fast, forward_slow)
    copy_cotn.wait()

    w2n_flip = flip(w2n_ref[...])
    w1n_flip = jnp.concatenate([flip(w1n_ref[0:H]), flip(w1n_ref[H : 2 * H])], axis=1)

    def cells(k, carry):
        at = pl.ds(pl.multiple_of(k * TILE, TILE), TILE)
        eu = eu_ref[at, :]
        usum = eu[:, H:]
        uh = usum.astype(BF16)
        ul = (usum - uh.astype(F32)).astype(BF16)
        w2 = w2e_ref[...]
        agg = (eu[:, 0:H] + deg_ref[at, :] * b2e_ref[...]) + dot(
            jnp.concatenate([uh, ul], axis=1), jnp.concatenate([w2, w2], axis=0)
        )
        x = jnp.concatenate([node_ref[at, :], agg.astype(BF16)], axis=1)
        z = dot(x, w1n_ref[...]) + b1n_ref[...]
        s = sigmoid(z)
        u = z * s
        cot = cotn_ref[at, :]
        dz = (dot(cot, w2n_flip) * (s + u * (1.0 - s))).astype(BF16)
        dx = dot(dz, w1n_flip)
        cot32 = cot.astype(F32)
        gown_ref[at, :] = cot32 + dx[:, 0:H]
        dagg = dx[:, H:].astype(BF16)
        dd_ref[at, 0:H] = dot(dagg, const_ref[:, 0:H])
        dd_ref[at, H:] = dx[:, H:]
        par_ref[4 * H : 6 * H, :] += dot_first(x, dz)
        par_ref[6 * H : 7 * H, :] += dot_first(u.astype(BF16), cot)
        par_ref[7 * H + 2 : 7 * H + 3, :] += jnp.sum(dz.astype(F32), axis=0, keepdims=True)
        par_ref[7 * H + 3 : 7 * H + 4, :] += jnp.sum(cot32, axis=0, keepdims=True)
        return carry

    lax.fori_loop(0, CELLS // TILE, cells, 0, unroll=8)
    copy_cot.wait()

    def spread(home, w, cot):
        left = jnp.concatenate([hot(home == lane + w), cot], axis=1)
        right = jnp.concatenate([dd_ref[pl.ds(w, H), :].astype(BF16), const_ref[...]], axis=0)
        return dot(left, right)

    def scatter(t, w, dz, guard):
        mid = mid_of(w)
        parts = []
        for place, home in zip(places(t), homes(t)):
            if guard:
                place = keep_near(place, home, w)
            parts.append(
                jnp.concatenate(
                    [
                        hot(place == mrow + mid),
                        hot(place == wrow + (w + 4096)),
                        hot(place == wrow + (w + 8192)),
                        hot(home == wrow + w),
                    ],
                    axis=0,
                )
            )
        sums = dot(jnp.concatenate(parts, axis=1), dz)
        smid_ref[pl.ds(mid, MID), :] += sums[0:MID]
        spad_ref[pl.ds(w + 2 * PLANE, WIN), :] += sums[MID : MID + WIN]
        spad_ref[pl.ds(w, WIN), :] += sums[MID + WIN : MID + 2 * WIN]
        rsum_ref[pl.ds(w, WIN), :] += sums[MID + 2 * WIN :]

    def finish_edges(t, dd):
        d32 = dd[:, H:]
        d = d32.astype(BF16)
        dz = (dd[:, 0:H] * slope_ref[rows_of(t), :].astype(F32)).astype(BF16)
        gedge_ref[rows_of(t), :] = (d32 + dot(dz, flip_ref[2 * H : 3 * H])).astype(BF16)
        wide_ref[0:H, :] += dot_first(e_ref[rows_of(t), :], dz)
        wide_ref[H : 2 * H, :] += dot_first(u_ref[rows_of(t), :], d)
        wide_ref[2 * H : 2 * H + 8, :] += jnp.sum(d32.reshape(TILE // 8, 8, H), axis=0)
        return dz

    def backward_fast(t):
        w = start_of(t)
        dz = finish_edges(t, spread(col_ref[rows_of(t), :], w, cot_ref[rows_of(t), :]))
        scatter(t, w, dz, False)

    def backward_slow(t):
        zacc_ref[...] = dot(cot_ref[rows_of(t), :], const_ref[...])

        def more(k, carry):
            w = pl.multiple_of(start_of(t) + k * H, 8)
            zacc_ref[...] += spread(
                col_ref[rows_of(t), :], w, jnp.zeros((TILE, H), BF16)
            )
            return carry

        lax.fori_loop(0, (windows_of(t) + 1) >> 1, more, 0)
        dz_ref[...] = finish_edges(t, zacc_ref[...])

        def put(k, carry):
            scatter(t, pl.multiple_of(start_of(t) + k * WIN, 8), dz_ref[...], True)
            return carry

        lax.fori_loop(0, windows_of(t), put, 0)

    per_chunk = TILES // GROUP // CHUNKS

    def send_out(g):
        @pl.when(g % per_chunk == per_chunk - 1)
        def _():
            copy_out(g // per_chunk).start()

    each_group(backward_fast, backward_slow, send_out)

    for i in range(N_PLANE):
        at = slice(i * PLANE, (i + 1) * PLANE)
        base = i * STRIDE
        for l in range(4):
            own_ref[pl.ds(i * PLANE + l, 32, 4), :] = smid_ref[pl.ds(base + 7 + l, 32, 6), :]
        zx_ref[0, i * 32 : (i + 1) * 32, :] = smid_ref[pl.ds(base + 6, 32, 6), :]
        zx_ref[1, i * 32 : (i + 1) * 32, :] = smid_ref[pl.ds(base + 11, 32, 6), :]
        nothing = jnp.zeros((4, H), F32)
        yx_ref[i * 8 : i * 8 + 8, :] = jnp.concatenate(
            [nothing, smid_ref[base + 1 : base + 5, :]], axis=0
        )
        yx_ref[PLANE + i * 8 : PLANE + i * 8 + 8, :] = jnp.concatenate(
            [smid_ref[base + 199 : base + 203, :], nothing], axis=0
        )

    def gather_cells(i, carry):
        base = pl.multiple_of(i * TILE, TILE)
        at = pl.ds(base, TILE)
        total = spad_ref[pl.ds(base + PLANE, TILE), :] + own_ref[at, :]
        sums = rsum_ref[at, :]
        par_ref[7 * H : 7 * H + 1, :] += jnp.sum(sums, axis=0, keepdims=True)
        sr16 = jnp.concatenate([total, sums], axis=1).astype(BF16)
        sr_ref[at, :] = sr16
        gown_ref[at, :] += dot(sr16, flip_ref[0 : 2 * H])
        return carry

    lax.fori_loop(0, CELLS // TILE, gather_cells, 0, unroll=8)
    both = dot_first(node_ref[...], sr_ref[...])
    w1b_flip = flip_ref[0:H]
    sx_lo = spad_ref[0:PLANE].astype(BF16)
    sx_hi = spad_ref[CELLS + PLANE : CELLS + 2 * PLANE].astype(BF16)
    sy_lo = yx_ref[0:PLANE].astype(BF16)
    sy_hi = yx_ref[PLANE : 2 * PLANE].astype(BF16)
    sz_lo = zx_ref[0].astype(BF16)
    sz_hi = zx_ref[1].astype(BF16)
    fxlo_ref[...] = dot(sx_lo, w1b_flip).astype(BF16)
    fxhi_ref[...] = dot(sx_hi, w1b_flip).astype(BF16)
    fylo_ref[...] = dot(sy_lo, w1b_flip).astype(BF16)
    fyhi_ref[...] = dot(sy_hi, w1b_flip).astype(BF16)
    fzlo_ref[...] = dot(sz_lo, w1b_flip).astype(BF16)
    fzhi_ref[...] = dot(sz_hi, w1b_flip).astype(BF16)
    halo_x = dot_first(xlo_ref[...], sx_lo) + dot_first(xhi_ref[...], sx_hi)
    halo_y = dot_first(ylo_ref[...], sy_lo) + dot_first(yhi_ref[...], sy_hi)
    halo_z = dot_first(zlo_ref[...], sz_lo) + dot_first(zhi_ref[...], sz_hi)
    par_ref[0:H, :] = wide_ref[0:H, :]
    par_ref[H : 2 * H, :] = both[:, 0:H] + halo_x + halo_y + halo_z
    par_ref[2 * H : 3 * H, :] = both[:, H:]
    par_ref[3 * H : 4 * H, :] = wide_ref[H : 2 * H, :]
    par_ref[7 * H + 1 : 7 * H + 2, :] = jnp.sum(
        wide_ref[2 * H : 2 * H + 8, :], axis=0, keepdims=True
    )
    par_out[...] = par_ref[...].astype(BF16)
    for c in range(CHUNKS):
        copy_out(c).wait()


def layer_call(senders, receivers, *arrays):
    smem = pl.BlockSpec(memory_space=pltpu.SMEM)
    vmem = pl.BlockSpec(memory_space=pltpu.VMEM)
    hbm = pl.BlockSpec(memory_space=pl.ANY)
    senders = senders.reshape(EDGES // H, H)
    receivers = receivers.reshape(EDGES // H, H)
    return pl.pallas_call(
        layer_kernel,
        in_specs=[smem] + [vmem] * 3 + [hbm] + [vmem] * 6 + [hbm] * 2 + [vmem] * 7,
        out_specs=[hbm] + [vmem] * 8,
        out_shape=[
            jax.ShapeDtypeStruct((EDGES, H), BF16),
            jax.ShapeDtypeStruct((CELLS, H), F32),
            jax.ShapeDtypeStruct((PLANE, H), BF16),
            jax.ShapeDtypeStruct((PLANE, H), BF16),
            jax.ShapeDtypeStruct((PLANE, H), BF16),
            jax.ShapeDtypeStruct((PLANE, H), BF16),
            jax.ShapeDtypeStruct((CELLS // 4, H), BF16),
            jax.ShapeDtypeStruct((CELLS // 4, H), BF16),
            jax.ShapeDtypeStruct((PARAM_ROWS, H), BF16),
        ],
        scratch_shapes=[
            pltpu.VMEM((EDGES, H), BF16),
            pltpu.VMEM((EDGES, H), BF16),
            pltpu.VMEM((CELLS, H), BF16),
            pltpu.VMEM((EDGES, H), BF16),
            pltpu.VMEM((TILE, H), BF16),
            pltpu.VMEM((CELLS, H), F32),
            pltpu.VMEM((2, CELLS // 4, H), F32),
            pltpu.VMEM((2 * PLANE, H), F32),
            pltpu.VMEM((PAD_ROWS, H), F32),
            pltpu.VMEM((ROWS, H), F32),
            pltpu.VMEM((GRID, H), F32),
            pltpu.VMEM((EDGES // H, H), jnp.int32),
            pltpu.VMEM((EDGES, H), jnp.int32),
            pltpu.VMEM((EDGES, H), BF16),
            pltpu.VMEM((EDGES, H), BF16),
            pltpu.VMEM((ROWS, 2 * H), F32),
            pltpu.VMEM((ROWS, H), F32),
            pltpu.VMEM((ROWS, 2 * H), F32),
            pltpu.VMEM((PAD_ROWS, H), F32),
            pltpu.VMEM((ROWS, H), F32),
            pltpu.VMEM((GRID, H), F32),
            pltpu.VMEM((2 * H + 8, H), F32),
            pltpu.VMEM((TILE, 2 * H), F32),
            pltpu.VMEM((H, 2 * H), BF16),
            pltpu.VMEM((3 * H, H), BF16),
            pltpu.VMEM((CELLS, 2 * H), BF16),
            pltpu.VMEM((PARAM_ROWS, H), F32),
            pltpu.SemaphoreType.DMA((3,)),
            pltpu.SemaphoreType.DMA((CHUNKS,)),
        ],
        compiler_params=pltpu.CompilerParams(vmem_limit_bytes=60 * 1024 * 1024),
        name="layer",
    )(receivers, senders, receivers, *arrays)


def node_kernel(
    gown_ref,
    xlo_ref,
    xhi_ref,
    ylo_ref,
    yhi_ref,
    zlo_ref,
    zhi_ref,
    gnode_ref,
    sum_ref,
):
    sum_ref[...] = gown_ref[...]
    sum_ref[0:PLANE] += xlo_ref[...].astype(F32)
    sum_ref[CELLS - PLANE :] += xhi_ref[...].astype(F32)
    for i in range(N_PLANE):
        low = ylo_ref[i * 8 : i * 8 + 8, :].astype(F32)
        high = yhi_ref[i * 8 : i * 8 + 8, :].astype(F32)
        sum_ref[i * PLANE : i * PLANE + 8, :] += low
        sum_ref[(i + 1) * PLANE - 8 : (i + 1) * PLANE, :] += high
    sum_ref[pl.ds(0, CELLS // 4, 4), :] += zlo_ref[...].astype(F32)
    sum_ref[pl.ds(3, CELLS // 4, 4), :] += zhi_ref[...].astype(F32)
    gnode_ref[...] = sum_ref[...].astype(BF16)


def node_call(*arrays):
    return pl.pallas_call(
        node_kernel,
        in_specs=[pl.BlockSpec(memory_space=pltpu.VMEM)] * 7,
        out_specs=pl.BlockSpec(memory_space=pltpu.VMEM),
        out_shape=jax.ShapeDtypeStruct((CELLS, H), BF16),
        scratch_shapes=[pltpu.VMEM((CELLS, H), F32)],
        name="nodes",
    )(*arrays)


def clip_kernel(par_ref, w1e_ref, w2e_ref, w1n_ref, w2n_ref, bias_ref):
    par = par_ref[0 : 7 * H + 16, :].astype(F32)
    square = jnp.sum(par * par)
    factor = 1.0 / jnp.maximum(1.0, jnp.sqrt(jnp.full((1, H), square / (7 * H * H + 4 * H), F32)))
    w1e_ref[...] = par[0 : 3 * H] * factor
    w2e_ref[...] = par[3 * H : 4 * H] * factor
    w1n_ref[...] = par[4 * H : 6 * H] * factor
    w2n_ref[...] = par[6 * H : 7 * H] * factor
    bias_ref[...] = par[7 * H : 7 * H + 4] * factor


def clip_call(par):
    return pl.pallas_call(
        clip_kernel,
        in_specs=[pl.BlockSpec(memory_space=pltpu.VMEM)],
        out_specs=[pl.BlockSpec(memory_space=pltpu.VMEM)] * 5,
        out_shape=[
            jax.ShapeDtypeStruct((3 * H, H), F32),
            jax.ShapeDtypeStruct((H, H), F32),
            jax.ShapeDtypeStruct((2 * H, H), F32),
            jax.ShapeDtypeStruct((H, H), F32),
            jax.ShapeDtypeStruct((4, H), F32),
        ],
        name="clip",
    )(par)


def from_previous(value, axis):
    n = lax.axis_size(axis)
    return lax.ppermute(value, axis, [(k, (k + 1) % n) for k in range(n)])


def from_next(value, axis):
    n = lax.axis_size(axis)
    return lax.ppermute(value, axis, [((k + 1) % n, k) for k in range(n)])


def sum_over_devices(rows):
    count = 1
    for axis in AXES:
        count *= lax.axis_size(axis)
    chunks = rows.reshape(count, -1, H)
    parts = lax.all_to_all(chunks, AXES, 0, 0, tiled=True)
    mine = jnp.sum(parts.astype(F32), axis=0).astype(BF16)
    copies = jnp.broadcast_to(mine[None], (count,) + mine.shape)
    return lax.all_to_all(copies, AXES, 0, 0, tiled=True).reshape(-1, H)


def on_device(
    node_latent,
    edge_latent,
    senders,
    receivers,
    w1_edge,
    b1_edge,
    w2_edge,
    b2_edge,
    w1_node,
    b1_node,
    w2_node,
    cot_node,
    cot_edge,
):
    ylo = from_previous(node_latent[:, 30:32], "gy").reshape(-1, H)
    zlo = from_previous(node_latent[:, :, 3], "gz").reshape(-1, H)
    xlo = from_previous(node_latent[15], "gx").reshape(-1, H)
    yhi = from_next(node_latent[:, 0:2], "gy").reshape(-1, H)
    zhi = from_next(node_latent[:, :, 0], "gz").reshape(-1, H)
    xhi = from_next(node_latent[0], "gx").reshape(-1, H)
    gedge, gown, fxlo, fxhi, fylo, fyhi, fzlo, fzhi, par = layer_call(
        senders,
        receivers,
        node_latent.reshape(CELLS, H),
        cot_node.reshape(CELLS, H),
        xlo,
        xhi,
        ylo,
        yhi,
        zlo,
        zhi,
        edge_latent.reshape(EDGES, H),
        cot_edge.reshape(EDGES, H),
        w1_edge,
        b1_edge.reshape(1, H),
        w2_edge,
        b2_edge.reshape(1, H),
        w1_node,
        b1_node.reshape(1, H),
        w2_node,
    )
    full = sum_over_devices(par)
    gzlo, gzhi = from_previous(fzhi, "gz"), from_next(fzlo, "gz")
    gxlo, gxhi = from_previous(fxhi, "gx"), from_next(fxlo, "gx")
    gylo, gyhi = from_previous(fyhi, "gy"), from_next(fylo, "gy")
    gnode = node_call(gown, gxlo, gxhi, gylo, gyhi, gzlo, gzhi)
    gw1e, gw2e, gw1n, gw2n, gbias = clip_call(full)
    return (
        gnode.reshape(node_latent.shape),
        gedge.reshape(edge_latent.shape),
        gw1e,
        gw2e,
        gw1n,
        gw2n,
        gbias,
    )


def solution(mesh):
    cells = P("gx", "gy", "gz", None)
    edges = P("gx", "gy", "gz", None, None)
    return jax.shard_map(
        on_device,
        mesh=mesh,
        in_specs=(cells, edges, cells, cells) + (P(),) * 7 + (cells, edges),
        out_specs=(cells, edges) + (P(),) * 5,
        check_vma=False,
    )
```
